128 devices in a mesh: slab: 16 (over z, x), tile: 8 (over y, core).
Axes of the slice: x: 4, y: 4, z: 4, core: 2. Of those that a mesh axis runs over, the one named last changes fastest.
Arguments:
- fixed_planes: float32 [512, 512, 128], P(('slab', 'tile')), may hold values from -6 to 6
- moving_planes: float32 [2, 512, 512, 128], P(None, ('slab', 'tile')), may hold values from -6 to 6
- pair_dest: int32 [2, 512], P(None, ('slab', 'tile')), may hold values from 0 to 15, as said below
- pair_slot: int32 [2, 512], P(None, ('slab', 'tile')), may hold values from 0 to 3, as said below
- plane_shift: int32 [2, 2, 512], P(None, None, ('slab', 'tile')), may hold values from -24 to 24
- live_count: int32 [128], P(('slab', 'tile')), may hold values from 1 to 4, 298 in all
- piece_block: int32 [8192], P(('slab', 'tile')), may hold values from 0 to 2047, as said below
Outputs:
- peaks: float32 [2, 512], P(None, ('slab', 'tile'))
- blocks: float32 [2048, 32, 128], P(('slab', 'tile'))
The draws below stay inside these ranges and needn't reach their ends.
Inputs may be any that keep to these rules, and one draw needn't show every extreme that they name: `pair_dest`: round 0 entries lie in 0 to 15 and round 1 entries in 0 to 7. With pair_slot, every fixed plane of every device is targeted by exactly one moving plane in each round. In round 0 no device targets more than 2 planes of any one device, in round 1 no more than 2; in every round every device targets exactly that many planes of some device. `pair_slot`: drawn together with pair_dest. `live_count`: the counts sum to 298 and some device has 4. `piece_block`: block b is owned by device b // 16 along slab+tile. At most 2 pieces of one device go to blocks of one owner, and the first 2 pieces of every device go to blocks of one owner.
All inputs are finite; a program needn't handle non-finite values.
Results may differ from the reference program's by a relative error of at most 0.0003.
Values sent between devices are 32-bit elements; how exact they have to be, the bound alone decides.
A program may use at most 128 MiB of HBM per device.

```python
import math
import jax
import jax.numpy as jnp
import numpy as np
from jax import lax

H = 512
W = 128
STRIPS = 4
PIECES = 16
OWNED = 16
PLANES = 512
BLOCKS = 2048
CAP_SLAB = 2
CAP_TILE = 2
ROUTE_CAP = 2
N_SLAB = 16
N_TILE = 8
DEVICES = 128


def group_matching(subkey, group_size, capacity):
    subkeys = jax.random.split(subkey, 7)
    full_bin = jax.random.randint(subkeys[0], (), 0, group_size)
    spread = jax.random.permutation(subkeys[1], (group_size - 1) * capacity)[:STRIPS - capacity]
    other_bins = spread // capacity
    other_bins = other_bins + (other_bins >= full_bin).astype(jnp.int32)
    bin_ids = lax.iota(jnp.int32, group_size)
    counts = capacity * (bin_ids == full_bin).astype(jnp.int32) + jnp.sum((other_bins[:, None] == bin_ids[None, :]).astype(jnp.int32), 0)
    offsets = jnp.cumsum(counts) - counts
    position = lax.iota(jnp.int32, STRIPS)
    inside = (position[:, None] >= offsets[None, :]) & (position[:, None] < (offsets + counts)[None, :])
    bin_of = jnp.sum(inside.astype(jnp.int32) * bin_ids[None, :], 1)
    row_order = jax.random.permutation(subkeys[2], group_size)
    column_order = jax.random.permutation(subkeys[3], group_size)
    relabel = jax.random.permutation(subkeys[4], group_size)
    orders = jax.vmap(lambda inner: jax.random.permutation(inner, STRIPS))(jax.random.split(subkeys[5], group_size))
    landings = jax.vmap(lambda inner: jax.random.permutation(inner, STRIPS))(jax.random.split(subkeys[6], group_size))
    bins_taken = bin_of[orders]
    target = relabel[(row_order[:, None] + column_order[bins_taken]) % group_size]
    landing = landings[target, orders]
    return (target.astype(jnp.int32), landing.astype(jnp.int32))


def matching(key):
    base = jax.random.fold_in(key, 4242)
    along_slab = jax.vmap(lambda inner: group_matching(inner, N_SLAB, CAP_SLAB))(jax.random.split(jax.random.fold_in(base, 1), N_TILE))
    along_tile = jax.vmap(lambda inner: group_matching(inner, N_TILE, CAP_TILE))(jax.random.split(jax.random.fold_in(base, 2), N_SLAB))
    first_target = jnp.transpose(along_slab[0], (1, 0, 2)).reshape(-1)
    first_landing = jnp.transpose(along_slab[1], (1, 0, 2)).reshape(-1)
    second_target = along_tile[0].reshape(-1)
    second_landing = along_tile[1].reshape(-1)
    return (jnp.stack([first_target, second_target]), jnp.stack([first_landing, second_landing]))


def draw_pair_dest(key, part):
    return matching(key)[0]


def draw_pair_slot(key, part):
    return matching(key)[1]


def owner_pieces(subkey):
    halves = jax.random.split(subkey, 2)
    slot_total = DEVICES * ROUTE_CAP
    order = jax.random.permutation(halves[0], slot_total)
    leader = order[0] // ROUTE_CAP
    ranks = lax.iota(jnp.int32, slot_total)
    score = jnp.where(order // ROUTE_CAP == leader, ranks - slot_total, ranks)
    arranged = order[jnp.argsort(score, stable=True)]
    picked = arranged[:STRIPS * PIECES]
    within = jax.random.randint(halves[1], (STRIPS * PIECES,), 0, OWNED)
    return (picked // ROUTE_CAP * OWNED + within).astype(jnp.int32)


def draw_piece_block(key, part):
    subkeys = jax.random.split(jax.random.fold_in(key, 9191), DEVICES)
    return jax.vmap(owner_pieces)(subkeys).reshape(-1)


def plant(values, stream_key, least, top_value):
    shape = values.shape
    place = [jax.random.randint(jax.random.fold_in(stream_key, axis), (), 0, shape[axis]) for axis in range(len(shape))]
    values = values.at[tuple(place)].set(least)
    longest = shape.index(max(shape))
    place[longest] = (place[longest] + 1) % shape[longest]
    return values.at[tuple(place)].set(top_value)


def steps_of(rng, shape, cuts, smallest, top_value):
    factor_of, own = 1.0, jax.random.fold_in(rng, 6)
    for axis_at, parts in cuts:
        heights = jnp.exp(jax.random.uniform(jax.random.fold_in(own, axis_at), (parts,), jnp.float32, smallest / len(cuts), top_value / len(cuts)))
        factor_of = factor_of * jnp.repeat(heights, shape[axis_at] // parts).reshape([-1 if axis == axis_at else 1 for axis in range(len(shape))])
    return factor_of


def length_profile(amount, total, most, slope):
    loads = [(1 << 20) // math.isqrt(grade ** slope) + 1 for grade in range(2, amount + 1)]
    surplus, holding = total - most - (amount - 1), [1] * (amount - 1)
    while surplus > 0:
        movable = [i for i in range(amount - 1) if holding[i] < most]
        mass, left = sum([loads[i] for i in movable]), surplus
        for i in movable:
            extra = min(most - holding[i], max(1, left * loads[i] // mass), surplus)
            holding[i] = holding[i] + extra
            surplus = surplus - extra
    return np.array([most] + holding)


def ragged_sizes(key, amount, total, reach, skew):
    if amount == 2:
        one = jax.random.randint(key, (), max(1, total - reach), min(reach, total - 1) + 1)
        return jnp.stack([one, total - one])
    lengths = jnp.asarray(length_profile(amount, total, reach, skew), jnp.int32)
    couples = (amount - 1) // 2
    source_of, receiver = lengths[1:1 + 2 * couples:2], lengths[2:2 + 2 * couples:2]
    margin = jnp.minimum(source_of - 1, reach - receiver)
    passed = jax.random.randint(jax.random.fold_in(key, 1), (couples,), 0, 1 << 20) % (margin + 1)
    lengths = lengths.at[1:1 + 2 * couples:2].set(source_of - passed).at[2:2 + 2 * couples:2].set(receiver + passed)
    return lengths[jax.random.permutation(jax.random.fold_in(key, 2), amount)]


def gaussian(stream_key, shape, deviation, limit, shards=(), kind=jnp.bfloat16):
    result = deviation * jax.random.normal(stream_key, shape, jnp.float32)
    if shards:
        result = result * steps_of(stream_key, shape, shards, -0.22, 0.18)
    return jnp.clip(result, -limit, limit).astype(kind)


def setup_inputs(seed: int = 0) -> dict:
    seeds = jax.random.split(jax.random.key(seed), 8)
    fixed_planes = gaussian(seeds[0], (PLANES, H, W), 1.0, 6.0, ((0, 128),), jnp.float32)
    moving_planes = gaussian(seeds[1], (2, PLANES, H, W), 1.0, 6.0, ((1, 128),), jnp.float32)
    pair_dest = draw_pair_dest(jax.random.fold_in(seeds[7], 71), 0)
    pair_slot = draw_pair_slot(jax.random.fold_in(seeds[7], 71), 0)
    plane_shift = plant(jax.random.randint(seeds[4], (2, 2, PLANES), -24, 25), jax.random.fold_in(seeds[4], 1), -24, 24).astype(jnp.int32)
    live_count = ragged_sizes(seeds[5], DEVICES, DEVICES * STRIPS * 7 // 12, STRIPS, 2).astype(jnp.int32)
    piece_block = draw_piece_block(jax.random.fold_in(seeds[7], 71), 0)
    return {"fixed_planes": fixed_planes, "moving_planes": moving_planes, "pair_dest": pair_dest, "pair_slot": pair_slot, "plane_shift": plane_shift, "live_count": live_count, "piece_block": piece_block}


FLOOR = 0.25
CENTER = 4.0

def correlate(spectrum, partner):
    moving_spectrum = jnp.fft.fft2(partner, norm='ortho')
    cross = spectrum * jnp.conj(moving_spectrum)
    magnitude = jnp.sqrt(jnp.real(cross) ** 2 + jnp.imag(cross) ** 2 + FLOOR ** 2)
    surface = jnp.real(jnp.fft.ifft2(cross / magnitude, norm='ortho'))
    return lax.optimization_barrier(jnp.max(surface, axis=(1, 2)))

def shift_planes(planes, downward, sideways):
    return jax.vmap(lambda plane, first_shift, second_shift: jnp.roll(plane, (first_shift, second_shift), axis=(0, 1)))(planes, downward, sideways)

def reference(fixed_planes, moving_planes, pair_dest, pair_slot, plane_shift, live_count, piece_block):
    plane_total = fixed_planes.shape[0]
    strip_index = jnp.arange(plane_total, dtype=jnp.int32)
    device = strip_index // STRIPS
    slab_place = device // N_TILE
    tile_place = device % N_TILE
    first_target = (pair_dest[0] * N_TILE + tile_place) * STRIPS + pair_slot[0]
    second_target = (slab_place * N_TILE + pair_dest[1]) * STRIPS + pair_slot[1]
    sources = [jnp.zeros((plane_total,), jnp.int32).at[target].set(strip_index) for target in (first_target, second_target)]

    def one_device(device_index):
        first_row = (device_index * STRIPS).astype(jnp.int32)
        fixed_part = lax.dynamic_slice_in_dim(fixed_planes, first_row, STRIPS, 0)
        spectrum = jnp.fft.fft2(fixed_part, norm='ortho')
        is_live = jnp.arange(STRIPS, dtype=jnp.int32) < live_count[device_index]
        weighted_sum = fixed_part
        weight_total = jnp.ones((STRIPS,), fixed_part.dtype)
        peak_list = []
        for round_index in range(2):
            chosen = lax.dynamic_slice_in_dim(sources[round_index], first_row, STRIPS, 0)
            partner = moving_planes[round_index][chosen]
            peak_value = correlate(spectrum, partner)
            weight = jax.nn.sigmoid(peak_value - CENTER)
            shifts = lax.dynamic_slice_in_dim(plane_shift[round_index], first_row, STRIPS, 1)
            weighted_sum = weighted_sum + weight[:, None, None] * shift_planes(partner, shifts[0], shifts[1])
            weight_total = weight_total + weight
            peak_list.append(jnp.where(is_live, peak_value, 0.0))
        return (jnp.stack(peak_list), weighted_sum / weight_total[:, None, None])
    peak_rows, merged = lax.map(one_device, jnp.arange(plane_total // STRIPS, dtype=jnp.int32))
    peaks = jnp.transpose(peak_rows, (1, 0, 2)).reshape(2, plane_total)
    band_rows = H // PIECES
    pieces = merged.reshape(plane_total * PIECES, band_rows, W)
    piece_index = jnp.arange(plane_total * PIECES, dtype=jnp.int32)
    piece_live = piece_index // PIECES % STRIPS < jnp.repeat(live_count, STRIPS * PIECES)
    kept_pieces = jnp.where(piece_live[:, None, None], pieces, 0.0)
    blocks = jax.ops.segment_sum(kept_pieces, piece_block, num_segments=BLOCKS)
    return (peaks, blocks)
```

```python
import functools
import math

import jax
import jax.numpy as jnp
import ml_dtypes
import numpy as np
from jax import lax
from jax.experimental import pallas as pl
from jax.experimental.pallas import tpu as pltpu
from jax.sharding import PartitionSpec as P

MESH = pl.DeviceIdType.MESH
F32 = jnp.float32
BF16 = jnp.bfloat16
H = 512
W = 128
STRIPS = 4
PIECES = 16
BAND = H // PIECES
OWNED = 16
HALF = H // 2
SPEC = HALF + 8
PAD = BAND + 8


def halves_of(table):
    high = table.astype(ml_dtypes.bfloat16)
    low = (table - high.astype(np.float64)).astype(ml_dtypes.bfloat16)
    return jnp.asarray(high), jnp.asarray(low)


def tables():
    n = np.arange(HALF)
    even = np.arange(0, HALF, 2)
    odd = np.arange(1, HALF, 2)
    row_scale = 1.0 / math.sqrt(H)

    def cos_rows(k):
        return np.cos(2 * np.pi * ((k[:, None] * n[None, :]) % H) / H) * row_scale

    def sin_rows(k):
        return np.sin(2 * np.pi * ((k[:, None] * n[None, :]) % H) / H) * row_scale

    last = np.zeros((8, HALF))
    last[0] = np.where(n % 2 == 0, 1.0, -1.0) * row_scale
    forward_even = np.concatenate([cos_rows(even), last, -sin_rows(even)], 0)
    forward_odd = np.concatenate([cos_rows(odd), -sin_rows(odd)], 0)
    re_part = 2 * cos_rows(even)
    re_part[0] *= 0.5
    im_part = -2 * sin_rows(even)
    im_part[0] = last[0]
    back_even = np.concatenate([re_part, im_part], 0).T
    back_odd = np.concatenate([2 * cos_rows(odd), -2 * sin_rows(odd)], 0).T
    m = np.arange(W)
    angle = 2 * np.pi * ((m[:, None] * m[None, :]) % W) / W
    c, s = np.cos(angle) / math.sqrt(W), np.sin(angle) / math.sqrt(W)
    column_forward = np.block([[c, -s], [s, c]])
    column_back = np.block([[c, s], [-s, c]])
    parts = []
    for table in (forward_even, forward_odd, column_forward, column_back, back_even, back_odd):
        parts.extend(halves_of(table))
    return parts


def split(x):
    high = x.astype(BF16)
    return high, (x - high.astype(F32)).astype(BF16)


def dot(a, b):
    return jnp.dot(a, b, preferred_element_type=F32)


def left(high, low, x):
    xh, xl = split(x)
    return dot(high[...], xh) + (dot(low[...], xh) + dot(high[...], xl))


def right(x, high, low):
    xh, xl = split(x)
    return dot(xh, high[...]) + (dot(xl, high[...]) + dot(xh, low[...]))


def exchange_kernel(
    slabs, tiles, moving, codes, partner, got0, got1, pick0, pick1, code0, code1, inv_v, inv_s,
    send_a, recv_a, send_b, recv_b, send_c, recv_c, own_sem,
):
    p = lax.axis_index("slab")
    q = lax.axis_index("tile")
    groups = (("slab", slabs, p, got0, pick0, code0), ("tile", tiles, q, got1, pick1, code1))

    barrier = pltpu.get_barrier_semaphore()
    for axis, size, me, _, _, _ in groups:
        for step in range(1, size):
            pl.semaphore_signal(
                barrier, inc=1, device_id={axis: lax.rem(me + step, size)}, device_id_type=MESH
            )
    pl.semaphore_wait(barrier, slabs + tiles - 2)

    def code_copy(r, step):
        axis, size, me, _, _, code = groups[r]
        peer = lax.rem(me + step, size)
        base = r * slabs + step
        return pltpu.make_async_remote_copy(
            src_ref=codes.at[r], dst_ref=code.at[me], send_sem=send_c.at[base],
            recv_sem=recv_c.at[base], device_id={axis: peer}, device_id_type=MESH,
        )

    def spread_copy(r, step):
        axis, size, me, got, _, _ = groups[r]
        peer = lax.rem(me + step, size)
        rows = H // size
        base = r * slabs + step
        return pltpu.make_async_remote_copy(
            src_ref=moving.at[r, :, pl.ds(pl.multiple_of(peer * rows, rows), rows), :],
            dst_ref=got.at[pl.ds(me * STRIPS, STRIPS)],
            send_sem=send_a.at[base], recv_sem=recv_a.at[base],
            device_id={axis: peer}, device_id_type=MESH,
        )

    def gather_copy(r, step):
        axis, size, me, _, pick, _ = groups[r]
        peer = lax.rem(me + step, size)
        rows = H // size
        base = r * slabs + step
        return pltpu.make_async_remote_copy(
            src_ref=pick.at[pl.ds(peer * STRIPS, STRIPS)],
            dst_ref=partner.at[r, :, pl.ds(pl.multiple_of(me * rows, rows), rows), :],
            send_sem=send_b.at[base], recv_sem=recv_b.at[base],
            device_id={axis: peer}, device_id_type=MESH,
        )

    own = []
    for r, (axis, size, me, got, _, code) in enumerate(groups):
        rows = H // size
        for step in range(1, size):
            code_copy(r, step).start()
        own.append(pltpu.make_async_copy(
            moving.at[r, :, pl.ds(pl.multiple_of(me * rows, rows), rows), :],
            got.at[pl.ds(me * STRIPS, STRIPS)], own_sem.at[r]))
        own.append(pltpu.make_async_copy(codes.at[r], code.at[me], own_sem.at[2 + r]))
    for copy in own:
        copy.start()
    for step in range(1, slabs):
        spread_copy(0, step).start()
        if step < tiles:
            spread_copy(1, step).start()

    for r, (axis, size, me, got, pick, code) in enumerate(groups):
        own[2 * r + 1].wait()
        for step in range(1, size):
            code_copy(r, step).wait()
        lane = lax.broadcasted_iota(jnp.int32, (8, W), 1)
        row = lax.broadcasted_iota(jnp.int32, (8, W), 0)
        total = jnp.zeros((8, W), jnp.int32)
        for i in range(size):
            total += jnp.where(code[i] == lane, i * STRIPS + row, 0)
        source = jnp.minimum(jnp.sum(total, 0, keepdims=True), size * STRIPS - 1)
        inv_v[r] = jnp.broadcast_to(source, (8, W))
    table = pltpu.make_async_copy(inv_v, inv_s, own_sem.at[4])
    table.start()
    table.wait()

    final = []
    for r in (1, 0):
        axis, size, me, got, pick, code = groups[r]
        rows = H // size
        own[2 * r].wait()
        for step in range(1, size):
            spread_copy(r, step).wait()
        for step in list(range(1, size)) + [0]:
            peer = lax.rem(me + step, size)
            for s in range(STRIPS):
                pick[peer * STRIPS + s] = got[inv_s[r, 0, peer * STRIPS + s]]
            if step:
                gather_copy(r, step).start()
        final.append(pltpu.make_async_copy(
            pick.at[pl.ds(me * STRIPS, STRIPS)],
            partner.at[r, :, pl.ds(pl.multiple_of(me * rows, rows), rows), :], own_sem.at[5 + r]))
        final[-1].start()
    for copy in final:
        copy.wait()
    for r in (1, 0):
        for step in range(1, groups[r][1]):
            gather_copy(r, step).wait()


def exchange(moving, codes, slabs, tiles):
    count = slabs + tiles
    return pl.pallas_call(
        functools.partial(exchange_kernel, slabs, tiles),
        out_shape=jax.ShapeDtypeStruct((2, STRIPS, H, W), F32),
        in_specs=[pl.BlockSpec(memory_space=pl.ANY), pl.BlockSpec(memory_space=pltpu.VMEM)],
        out_specs=pl.BlockSpec(memory_space=pl.ANY),
        scratch_shapes=[
            pltpu.VMEM((slabs * STRIPS, H // slabs, W), F32),
            pltpu.VMEM((tiles * STRIPS, H // tiles, W), F32),
            pltpu.VMEM((slabs * STRIPS, H // slabs, W), F32),
            pltpu.VMEM((tiles * STRIPS, H // tiles, W), F32),
            pltpu.VMEM((slabs, 8, W), jnp.int32),
            pltpu.VMEM((tiles, 8, W), jnp.int32),
            pltpu.VMEM((2, 8, W), jnp.int32),
            pltpu.SMEM((2, 8, W), jnp.int32),
        ]
        + [pltpu.SemaphoreType.DMA((count,))] * 6
        + [pltpu.SemaphoreType.DMA((8,))],
        compiler_params=pltpu.CompilerParams(collective_id=0, has_side_effects=True),
        name="exchange_rounds",
    )(moving, codes)


def merge_kernel(
    shifts, live, fixed, partner, fe_h, fe_l, fo_h, fo_l, cf_h, cf_l, cb_h, cb_l, be_h, be_l,
    bo_h, bo_l, peaks, spread, merged,
):
    s = pl.program_id(0)
    x = jnp.concatenate([fixed[0], partner[0, 0], partner[1, 0]], 1)
    u = left(fe_h, fe_l, x[:HALF] + x[HALF:])
    v = left(fo_h, fo_l, x[:HALF] - x[HALF:])
    quarter = HALF // 2
    joined = []
    for i in range(3):
        lanes = slice(W * i, W * (i + 1))
        re_part = jnp.concatenate(
            [u[:quarter, lanes], v[:quarter, lanes], u[quarter : quarter + 8, lanes]], 0)
        im_part = jnp.concatenate(
            [u[quarter + 8 :, lanes], v[quarter:, lanes], jnp.zeros((8, W), F32)], 0)
        joined.append(jnp.concatenate([re_part, im_part], 1))
    spectra = right(jnp.concatenate(joined, 0), cf_h, cf_l)
    fr, fi = spectra[:SPEC, :W], spectra[:SPEC, W:]
    crossed = []
    for i in (1, 2):
        gr, gi = spectra[SPEC * i : SPEC * (i + 1), :W], spectra[SPEC * i : SPEC * (i + 1), W:]
        cr = fr * gr + fi * gi
        ci = fi * gr - fr * gi
        scale = lax.rsqrt(cr * cr + ci * ci + 0.0625)
        crossed.append(jnp.concatenate([cr * scale, ci * scale], 1))
    back = right(jnp.concatenate(crossed, 0), cb_h, cb_l)
    evens, odds = [], []
    first = lax.broadcasted_iota(jnp.int32, (8, W), 0) == 0
    for i in range(2):
        pr, pi = back[SPEC * i : SPEC * (i + 1), :W], back[SPEC * i : SPEC * (i + 1), W:]
        evens.append(jnp.concatenate(
            [pr[:quarter], jnp.where(first, pr[HALF:], pi[:8]), pi[8:quarter]], 0))
        odds.append(jnp.concatenate([pr[quarter:HALF], pi[quarter:HALF]], 0))
    even = left(be_h, be_l, jnp.concatenate(evens, 1))
    odd = left(bo_h, bo_l, jnp.concatenate(odds, 1))
    surface = even + jnp.abs(odd)
    is_live = s < live[0]
    total = jnp.ones((1, 1), F32)
    acc = fixed[0]
    for r in range(2):
        peak = jnp.max(surface[:, W * r : W * (r + 1)], axis=(0, 1), keepdims=True)
        weight = 1.0 / (1.0 + jnp.exp(4.0 - peak))
        down = lax.rem(shifts[r, 0, s] + H, H)
        side = lax.rem(shifts[r, 1, s] + W, W)
        moved = pltpu.roll(pltpu.roll(partner[r, 0], side, 1), down, 0)
        acc = acc + weight * moved
        total = total + weight
        peaks[0, r : r + 1, :] = jnp.broadcast_to(jnp.where(is_live, peak, 0.0), (1, W))
    peaks[0, 2:8, :] = jnp.zeros((6, W), F32)
    acc = jnp.where(is_live, acc * (1.0 / total), 0.0)
    for k in range(PIECES):
        merged[pl.ds(k * PAD, BAND), :] = acc[k * BAND : (k + 1) * BAND]
    for r in range(BAND):
        spread[r] = merged[pl.ds(r, PIECES, stride=PAD), :]


def merge(shifts, live, fixed, partner):
    parts = tables()
    whole = lambda t: pl.BlockSpec(t.shape, lambda s: (0, 0))
    return pl.pallas_call(
        merge_kernel,
        grid=(STRIPS,),
        out_shape=(
            jax.ShapeDtypeStruct((STRIPS, 8, W), F32),
            jax.ShapeDtypeStruct((BAND, STRIPS * PIECES, W), F32),
        ),
        in_specs=[
            pl.BlockSpec(memory_space=pltpu.SMEM),
            pl.BlockSpec(memory_space=pltpu.SMEM),
            pl.BlockSpec((1, H, W), lambda s: (s, 0, 0)),
            pl.BlockSpec((2, 1, H, W), lambda s: (0, s, 0, 0)),
        ]
        + [whole(t) for t in parts],
        out_specs=(
            pl.BlockSpec((1, 8, W), lambda s: (s, 0, 0)),
            pl.BlockSpec((BAND, PIECES, W), lambda s: (0, s, 0)),
        ),
        scratch_shapes=[pltpu.VMEM((PIECES * PAD, W), F32)],
        name="correlate_merge",
    )(shifts, live, fixed, partner, *parts)


def rows_kernel(slabs, tiles, inner, spread, labels, got, got_labels, send_a, recv_a, send_b, recv_b, own_sem):
    p = lax.axis_index("slab")
    q = lax.axis_index("tile")
    size = inner * tiles
    base = (p // inner) * inner
    me = lax.rem(p, inner) * tiles + q

    def place(step):
        peer = lax.rem(me + step, size)
        return peer, (base + peer // tiles, lax.rem(peer, tiles))

    barrier = pltpu.get_barrier_semaphore()
    for step in range(1, size):
        pl.semaphore_signal(barrier, inc=1, device_id=place(step)[1], device_id_type=MESH)
    pl.semaphore_wait(barrier, size - 1)

    def data(step):
        peer, device = place(step)
        return pltpu.make_async_remote_copy(
            src_ref=spread.at[peer], dst_ref=got.at[me], send_sem=send_a.at[step],
            recv_sem=recv_a.at[step], device_id=device, device_id_type=MESH)

    def label(step):
        _, device = place(step)
        return pltpu.make_async_remote_copy(
            src_ref=labels, dst_ref=got_labels.at[me], send_sem=send_b.at[step],
            recv_sem=recv_b.at[step], device_id=device, device_id_type=MESH)

    own_data = pltpu.make_async_copy(spread.at[me], got.at[me], own_sem.at[0])
    own_label = pltpu.make_async_copy(labels, got_labels.at[me], own_sem.at[1])
    for step in range(1, size):
        label(step).start()
        data(step).start()
    own_data.start()
    own_label.start()
    own_data.wait()
    own_label.wait()
    for step in range(1, size):
        label(step).wait()
        data(step).wait()


def rows_exchange(spread, labels, slabs, tiles):
    inner = BAND // tiles
    return pl.pallas_call(
        functools.partial(rows_kernel, slabs, tiles, inner),
        out_shape=(
            jax.ShapeDtypeStruct((BAND, STRIPS * PIECES, W), F32),
            jax.ShapeDtypeStruct((BAND, 1, W), jnp.int32),
        ),
        in_specs=[pl.BlockSpec(memory_space=pltpu.VMEM), pl.BlockSpec(memory_space=pltpu.VMEM)],
        out_specs=(pl.BlockSpec(memory_space=pltpu.VMEM), pl.BlockSpec(memory_space=pltpu.VMEM)),
        scratch_shapes=[pltpu.SemaphoreType.DMA((BAND,))] * 4 + [pltpu.SemaphoreType.DMA((2,))],
        compiler_params=pltpu.CompilerParams(collective_id=1, has_side_effects=True),
        name="spread_rows",
    )(spread, labels)


BANKS = 8


def sum_kernel(got, labels, sums, *banks):
    blocks = sums.shape[0]
    zero = jnp.zeros((64, W), F32)

    def clear(i, carry):
        for bank in banks:
            bank[pl.ds(pl.multiple_of(i * 64, 64), 64), :] = zero
        return carry

    lax.fori_loop(0, blocks // 64, clear, 0)
    per = got.shape[1] // BANKS

    def add(i, carry):
        d = i // per
        k = lax.rem(i, per) * BANKS
        for b, bank in enumerate(banks):
            block = labels[d, 0, k + b]
            bank[pl.ds(block, 1), :] += got[d, pl.ds(k + b, 1), :]
        return carry

    lax.fori_loop(0, got.shape[0] * per, add, 0)

    def fold(i, carry):
        at = pl.ds(pl.multiple_of(i * 64, 64), 64)
        parts = [bank[at, :] for bank in banks]
        while len(parts) > 1:
            parts = [parts[j] + parts[j + 1] for j in range(0, len(parts), 2)]
        sums[at, :] = parts[0]
        return carry

    lax.fori_loop(0, blocks // 64, fold, 0)


def sum_blocks(got, labels, blocks):
    return pl.pallas_call(
        sum_kernel,
        out_shape=jax.ShapeDtypeStruct((blocks, W), F32),
        in_specs=[pl.BlockSpec(memory_space=pltpu.VMEM), pl.BlockSpec(memory_space=pltpu.SMEM)],
        out_specs=pl.BlockSpec(memory_space=pltpu.VMEM),
        scratch_shapes=[pltpu.VMEM((blocks, W), F32)] * BANKS,
        name="sum_blocks",
    )(got, labels)


def owners_kernel(slabs, tiles, sums, out, got, send_sem, recv_sem, own_sem):
    p = lax.axis_index("slab")
    q = lax.axis_index("tile")
    size = slabs * tiles
    me = p * tiles + q

    def place(step):
        peer = lax.rem(me + step, size)
        return peer, (peer // tiles, lax.rem(peer, tiles))

    barrier = pltpu.get_barrier_semaphore()

    def greet(step, carry):
        pl.semaphore_signal(barrier, inc=1, device_id=place(step)[1], device_id_type=MESH)
        return carry

    lax.fori_loop(1, size, greet, 0)
    pl.semaphore_wait(barrier, size - 1)

    def copy(step):
        peer, device = place(step)
        return pltpu.make_async_remote_copy(
            src_ref=sums.at[peer], dst_ref=got.at[me], send_sem=send_sem.at[step],
            recv_sem=recv_sem.at[step], device_id=device, device_id_type=MESH)

    def start(step, carry):
        copy(step).start()
        return carry

    def wait(step, carry):
        copy(step).wait()
        return carry

    lax.fori_loop(1, size, start, 0)
    got[me] = sums[me]
    lax.fori_loop(1, size, wait, 0)
    for r in range(BAND):
        total = got[r]
        for z in range(1, size // BAND):
            total = total + got[z * BAND + r]
        out[:, r, :] = total


def to_owners(sums, slabs, tiles):
    size = slabs * tiles
    return pl.pallas_call(
        functools.partial(owners_kernel, slabs, tiles),
        out_shape=jax.ShapeDtypeStruct((OWNED, BAND, W), F32),
        in_specs=[pl.BlockSpec(memory_space=pltpu.VMEM)],
        out_specs=pl.BlockSpec(memory_space=pltpu.VMEM),
        scratch_shapes=[
            pltpu.VMEM((size, OWNED, W), F32),
            pltpu.SemaphoreType.DMA((size,)),
            pltpu.SemaphoreType.DMA((size,)),
            pltpu.SemaphoreType.DMA((1,)),
        ],
        compiler_params=pltpu.CompilerParams(collective_id=2, has_side_effects=True),
        name="rows_to_owners",
    )(sums)


def local(slabs, tiles, fixed, moving, pair_dest, pair_slot, plane_shift, live_count, piece_block):
    codes = pair_dest * STRIPS + pair_slot
    codes = jnp.concatenate([codes, jnp.full((2, 8 - STRIPS), -1, jnp.int32)], 1)
    codes = jnp.broadcast_to(codes[:, :, None], (2, 8, W))
    partner = exchange(moving, codes, slabs, tiles)
    peaks, spread = merge(plane_shift, live_count, fixed, partner)
    labels = jnp.pad(piece_block, (0, W - piece_block.shape[0])).reshape(1, W)
    got, got_labels = rows_exchange(spread, labels, slabs, tiles)
    size = slabs * tiles
    sums = sum_blocks(got, got_labels, size * OWNED)
    blocks = to_owners(sums.reshape(size, OWNED, W), slabs, tiles)
    return peaks[:, :2, 0].T, blocks


def solution(mesh):
    both = ("slab", "tile")
    placed = (
        P(both, None, None),
        P(None, both, None, None),
        P(None, both),
        P(None, both),
        P(None, None, both),
        P(both),
        P(both),
    )
    return jax.shard_map(
        functools.partial(local, mesh.shape["slab"], mesh.shape["tile"]),
        mesh=mesh,
        in_specs=placed,
        out_specs=(P(None, both), P(both, None, None)),
        check_vma=False,
    )
```

```python
import functools
import math

import jax
import jax.numpy as jnp
import ml_dtypes
import numpy as np
from jax import lax
from jax.experimental import pallas as pl
from jax.experimental.pallas import tpu as pltpu
from jax.sharding import PartitionSpec as P

MESH = pl.DeviceIdType.MESH
F32 = jnp.float32
BF16 = jnp.bfloat16
H = 512
W = 128
STRIPS = 4
PIECES = 16
BAND = H // PIECES
OWNED = 16
HALF = H // 2
QUARTER = HALF // 2
SPEC = HALF + 8
PAD = BAND + 8
RING = 4
FIRST = HALF + 16


def tables():
    n = np.arange(HALF)
    even = np.arange(0, HALF, 2)
    odd = np.arange(1, HALF, 2)
    row_scale = 1.0 / math.sqrt(H)

    def cos_rows(k):
        return np.cos(2 * np.pi * ((k[:, None] * n[None, :]) % H) / H) * row_scale

    def sin_rows(k):
        return np.sin(2 * np.pi * ((k[:, None] * n[None, :]) % H) / H) * row_scale

    last = np.zeros((16, HALF))
    last[0] = np.where(n % 2 == 0, 1.0, -1.0) * row_scale
    forward_even = np.concatenate([cos_rows(even), last, -sin_rows(even)], 0)
    forward_odd = np.concatenate([cos_rows(odd), -sin_rows(odd)], 0)
    re_part = 2 * cos_rows(even)
    re_part[0] *= 0.5
    im_part = -2 * sin_rows(even)
    im_part[0] = last[0]
    back_even = np.concatenate([re_part, im_part], 0).T
    back_odd = np.concatenate([2 * cos_rows(odd), -2 * sin_rows(odd)], 0).T
    m = np.arange(W)
    angle = 2 * np.pi * ((m[:, None] * m[None, :]) % W) / W
    c, s = np.cos(angle) / math.sqrt(W), np.sin(angle) / math.sqrt(W)
    column_forward = np.block([[c, -s], [s, c]])
    column_back = np.block([[c, s], [-s, c]])
    table = np.concatenate(
        [forward_even, forward_odd, column_forward, column_back, back_even, back_odd], 0
    )
    high = table.astype(ml_dtypes.bfloat16)
    low = (table - high.astype(np.float64)).astype(ml_dtypes.bfloat16)
    return jnp.asarray(np.stack([high, low]))


TABLE_ROWS = FIRST + 5 * HALF


def dot(a, b):
    return jnp.dot(a, b, preferred_element_type=F32)


def split(x):
    high = x.astype(BF16)
    return high, (x - high.astype(F32)).astype(BF16)


def part(table, index):
    start, rows = (0, FIRST) if index == 0 else (FIRST + HALF * (index - 1), HALF)
    return table[0, start : start + rows, :], table[1, start : start + rows, :]


def left(table, index, x):
    high, low = part(table, index)
    xh, xl = split(x)
    return dot(high, xh) + (dot(low, xh) + dot(high, xl))


def right(x, table, index):
    high, low = part(table, index)
    xh, xl = split(x)
    return dot(xh, high) + (dot(xl, high) + dot(xh, low))


def forward_pair(table, a, b):
    x = jnp.concatenate([a, b], 1)
    u = left(table, 0, x[:HALF] + x[HALF:])
    v = left(table, 1, x[:HALF] - x[HALF:])
    joined = []
    for i in range(2):
        lanes = slice(W * i, W * (i + 1))
        re_part = jnp.concatenate(
            [u[:QUARTER, lanes], v[:QUARTER, lanes], u[QUARTER : QUARTER + 8, lanes]], 0)
        im_part = jnp.concatenate(
            [u[QUARTER + 16 :, lanes], v[QUARTER:, lanes], jnp.zeros((8, W), F32)], 0)
        joined.append(jnp.concatenate([re_part, im_part], 1))
    return right(jnp.concatenate(joined, 0), table, 2)


def surfaces(table, fixed_spectrum, spectra):
    fr, fi = fixed_spectrum[:, :W], fixed_spectrum[:, W:]
    crossed = []
    for i in range(2):
        gr, gi = spectra[SPEC * i : SPEC * (i + 1), :W], spectra[SPEC * i : SPEC * (i + 1), W:]
        cr = fr * gr + fi * gi
        ci = fi * gr - fr * gi
        scale = lax.rsqrt(cr * cr + ci * ci + 0.0625)
        crossed.append(jnp.concatenate([cr * scale, ci * scale], 1))
    back = right(jnp.concatenate(crossed, 0), table, 3)
    evens, odds = [], []
    first = lax.broadcasted_iota(jnp.int32, (8, W), 0) == 0
    for i in range(2):
        pr, pi = back[SPEC * i : SPEC * (i + 1), :W], back[SPEC * i : SPEC * (i + 1), W:]
        evens.append(jnp.concatenate(
            [pr[:QUARTER], jnp.where(first, pr[HALF:], pi[:8]), pi[8:QUARTER]], 0))
        odds.append(jnp.concatenate([pr[QUARTER:HALF], pi[QUARTER:HALF]], 0))
    even = left(table, 4, jnp.concatenate(evens, 1))
    odd = left(table, 5, jnp.concatenate(odds, 1))
    return even + jnp.abs(odd)


def far_first(*sizes):
    grid = [[]]
    for size in sizes:
        grid = [g + [v] for g in grid for v in range(size)]
    grid = [tuple(g) for g in grid if any(g)]

    def hops(g):
        return sum(min(v, RING - v) for v in g[:-1]) + (
            min(g[-1], RING - g[-1]) if sizes[-1] == RING else 0.25 * g[-1])

    return sorted(grid, key=lambda g: (-hops(g), g))


def whole_kernel(
    slabs, tiles, dest, slot, shifts, live, labels, moving, fixed_in, table_in, peaks, out,
    fixed, table, got0, got1, pick0, pick1, partner, code0, code1, inv_v, inv_s, fixed_spec,
    merged, spread, rows_got, label_got, onehot, sums, owned,
    send_sem, spread_sem, code_sem, label_sem, slot_sem, rows_sem, own_sem, owner_sem, ready,
):
    p = lax.axis_index("slab")
    q = lax.axis_index("tile")
    z, x = p // RING, lax.rem(p, RING)
    y, c = q // 2, lax.rem(q, 2)
    me = p * tiles + q
    member = lax.rem(me, BAND)
    devices = slabs * tiles
    axes = ("slab", "tile")
    sizes = (slabs, tiles)
    mine = (p, q)
    got = (got0, got1)
    pick = (pick0, pick1)
    code = (code0, code1)
    rows = (H // slabs, H // tiles)

    def slab_peer(g):
        return lax.rem(z + g[0], RING) * RING + lax.rem(x + g[1], RING)

    def tile_peer(g):
        return lax.rem(y + g[0], RING) * 2 + lax.rem(c + g[1], 2)

    peers = (
        [slab_peer(g) for g in far_first(RING, RING)],
        [tile_peer(g) for g in far_first(RING, 2)],
    )

    def local_wait(ref, sem):
        pltpu.make_async_copy(ref, ref, sem).wait()

    row8 = lax.broadcasted_iota(jnp.int32, (8, W), 0)
    lane8 = lax.broadcasted_iota(jnp.int32, (8, W), 1)

    barrier = pltpu.get_barrier_semaphore()
    for r in range(2):
        for peer in peers[r]:
            pl.semaphore_signal(barrier, inc=1, device_id={axes[r]: peer}, device_id_type=MESH)
    for r in range(2):
        tile = jnp.full((8, W), -1, jnp.int32)
        for s in range(STRIPS):
            tile = jnp.where(row8 == s, dest[r, s] * STRIPS + slot[r, s], tile)
        code[r][mine[r]] = tile
    label_got[member] = pltpu.roll(labels[...], lax.rem(member, 8) * PIECES, 1)
    pl.semaphore_wait(barrier, slabs + tiles - 2)

    for r in range(2):
        for peer in peers[r]:
            pltpu.make_async_remote_copy(
                src_ref=code[r].at[mine[r]], dst_ref=code[r].at[mine[r]],
                send_sem=send_sem.at[r], recv_sem=code_sem.at[r],
                device_id={axes[r]: peer}, device_id_type=MESH,
            ).start()

    def spread_start(r, i):
        peer = peers[r][i]
        pltpu.make_async_remote_copy(
            src_ref=moving.at[r, :, pl.ds(pl.multiple_of(peer * rows[r], rows[r]), rows[r]), :],
            dst_ref=got[r].at[pl.ds(mine[r] * STRIPS, STRIPS)],
            send_sem=send_sem.at[2 + r], recv_sem=spread_sem.at[r],
            device_id={axes[r]: peer}, device_id_type=MESH,
        ).start()

    for i in range(slabs - 1):
        spread_start(0, i)
        if i % 2 == 0 and i // 2 < tiles - 1:
            spread_start(1, i // 2)
    own = [
        pltpu.make_async_copy(
            moving.at[r, :, pl.ds(pl.multiple_of(mine[r] * rows[r], rows[r]), rows[r]), :],
            got[r].at[pl.ds(mine[r] * STRIPS, STRIPS)], own_sem.at[r])
        for r in range(2)
    ]
    load_fixed = pltpu.make_async_copy(fixed_in, fixed, own_sem.at[2])
    load_table = pltpu.make_async_copy(table_in, table, own_sem.at[3])
    load_fixed.start()
    load_table.start()
    for copy in own:
        copy.start()
    for peer in peers[0]:
        pl.semaphore_signal(ready, inc=1, device_id={"slab": peer}, device_id_type=MESH)

    for r in range(2):
        local_wait(code[r].at[pl.ds(0, sizes[r] - 1)], code_sem.at[r])
        total = jnp.zeros((8, W), jnp.int32)
        for i in range(sizes[r]):
            total += jnp.where(code[r][i] == lane8, i * STRIPS + row8, 0)
        source = jnp.minimum(jnp.sum(total, 0, keepdims=True), sizes[r] * STRIPS - 1)
        inv_v[r] = jnp.broadcast_to(source, (8, W))
    to_scalars = pltpu.make_async_copy(inv_v, inv_s, own_sem.at[4])
    to_scalars.start()

    pl.semaphore_wait(ready, slabs - 1)
    group_base = (p // (BAND // tiles)) * (BAND // tiles)

    def group_peer(step):
        peer = lax.rem(member + step, BAND)
        return peer, (group_base + peer // tiles, lax.rem(peer, tiles))

    def send_label(step, carry):
        pltpu.make_async_remote_copy(
            src_ref=label_got.at[member], dst_ref=label_got.at[member],
            send_sem=send_sem.at[4], recv_sem=label_sem,
            device_id=group_peer(step)[1], device_id_type=MESH,
        ).start()
        return carry

    lax.fori_loop(1, BAND, send_label, 0)

    load_fixed.wait()
    load_table.wait()

    def fixed_pair(i, carry):
        spectra = forward_pair(table, fixed[2 * i], fixed[2 * i + 1])
        fixed_spec[2 * i] = spectra[:SPEC]
        fixed_spec[2 * i + 1] = spectra[SPEC:]
        return carry

    lax.fori_loop(0, STRIPS // 2, fixed_pair, 0)

    local_wait(label_got.at[pl.ds(0, BAND - 1)], label_sem)
    columns = []
    for g in range(BAND // 8):
        total = label_got[8 * g]
        for d in range(1, 8):
            total = total + label_got[8 * g + d]
        columns.append(total)
    chunk = 256
    for s in range(STRIPS):
        def build(i, carry):
            for g in range(BAND // 8):
                want = lax.broadcasted_iota(jnp.int32, (chunk, W), 0) + i * chunk
                hit = jnp.broadcast_to(columns[g][s : s + 1], (chunk, W)) == want
                onehot[s, pl.ds(pl.multiple_of(i * chunk, chunk), chunk), W * g : W * (g + 1)] = (
                    jnp.where(hit, 1.0, 0.0).astype(BF16))
            return carry

        lax.fori_loop(0, devices * OWNED // chunk, build, 0)

    to_scalars.wait()
    for r in (1, 0):
        own[r].wait()
        local_wait(got[r].at[pl.ds(0, (sizes[r] - 1) * STRIPS)], spread_sem.at[r])

    def choose(s, carry):
        for r in (0, 1):
            place = pl.ds(pl.multiple_of(mine[r] * rows[r], rows[r]), rows[r])
            partner[r, s, place, :] = got[r][inv_s[r, 0, mine[r] * STRIPS + s]]
            for peer in peers[r]:
                pick[r][s, peer] = got[r][inv_s[r, 0, peer * STRIPS + s]]
        for r in (0, 1):
            place = pl.ds(pl.multiple_of(mine[r] * rows[r], rows[r]), rows[r])
            for peer in peers[r]:
                pltpu.make_async_remote_copy(
                    src_ref=pick[r].at[s, peer], dst_ref=partner.at[r, s, place, :],
                    send_sem=send_sem.at[5 + r], recv_sem=slot_sem.at[r, s],
                    device_id={axes[r]: peer}, device_id_type=MESH,
                ).start()
        return carry

    lax.fori_loop(0, STRIPS, choose, 0)

    def correlate(s, found):
        for r in range(2):
            local_wait(partner.at[r, s, pl.ds(0, H - rows[r])], slot_sem.at[r, s])
        spectra = forward_pair(table, partner[0, s], partner[1, s])
        surface = surfaces(table, fixed_spec[s], spectra)
        is_live = s < live[0]
        total = jnp.ones((1, 1), F32)
        acc = fixed[s]
        for r in range(2):
            peak = jnp.max(surface[:, W * r : W * (r + 1)], axis=(0, 1), keepdims=True)
            weight = 1.0 / (1.0 + jnp.exp(4.0 - peak))
            down = lax.rem(shifts[r, 0, s] + H, H)
            side = lax.rem(shifts[r, 1, s] + W, W)
            moved = pltpu.roll(pltpu.roll(partner[r, s], side, 1), down, 0)
            acc = acc + weight * moved
            total = total + weight
            shown = jnp.where(is_live, peak, 0.0)
            found = jnp.where((row8 == r) & (lane8 == s), shown, found)
        acc = jnp.where(is_live, acc * (1.0 / total), 0.0)
        for k in range(PIECES):
            merged[pl.ds(k * PAD, BAND), :] = acc[k * BAND : (k + 1) * BAND]
        here = pl.ds(pl.multiple_of(s * PIECES, PIECES), PIECES)
        for r in range(BAND):
            spread[s, r] = merged[pl.ds(r, PIECES, stride=PAD), :]
        rows_got[s, member] = spread[s, member]

        def send_rows(step, carry):
            peer, device = group_peer(step)
            pltpu.make_async_remote_copy(
                src_ref=spread.at[s, peer], dst_ref=rows_got.at[s, member],
                send_sem=send_sem.at[7], recv_sem=rows_sem.at[s],
                device_id=device, device_id_type=MESH,
            ).start()
            return carry

        lax.fori_loop(1, BAND, send_rows, 0)
        return found

    found = lax.fori_loop(0, STRIPS, correlate, jnp.zeros((8, W), F32))
    peaks[...] = found[:2, :STRIPS]

    for s in range(STRIPS):
        local_wait(rows_got.at[s, pl.ds(0, BAND - 1)], rows_sem.at[s])
        high, low = split(rows_got[s].reshape(BAND * PIECES, W))
        both = jnp.concatenate([high, low], 1)

        def add(i, carry):
            at = pl.ds(pl.multiple_of(i * chunk, chunk), chunk)
            parts = dot(onehot[s, at, :], both)
            part_sum = (parts[:, :W] + parts[:, W:]).reshape(chunk // OWNED, OWNED, W)
            owners = pl.ds(i * (chunk // OWNED), chunk // OWNED)
            if s == 0:
                sums[owners] = part_sum
            else:
                sums[owners] += part_sum
            return carry

        lax.fori_loop(0, devices * OWNED // chunk, add, 0)

    def send_owner(k, carry):
        oz = lax.rem(z + 2 + k // 32, RING)
        ox = lax.rem(x + 2 + lax.rem(k // 8, RING), RING)
        oy = lax.rem(y + 2 + lax.rem(k // 2, RING), RING)
        oc = lax.rem(c + lax.rem(k, 2), 2)
        op, oq = oz * RING + ox, oy * 2 + oc
        pltpu.make_async_remote_copy(
            src_ref=sums.at[op * tiles + oq], dst_ref=owned.at[me],
            send_sem=send_sem.at[8], recv_sem=owner_sem,
            device_id=(op, oq), device_id_type=MESH,
        ).start()
        return carry

    self_at = 2 * 32 + 2 * 8 + 2 * 2
    lax.fori_loop(0, self_at, send_owner, 0)
    lax.fori_loop(self_at + 1, devices, send_owner, 0)
    owned[me] = sums[me]

    for r in range(2):
        local_wait(code[r].at[pl.ds(0, sizes[r] - 1)], send_sem.at[r])
        local_wait(got[r].at[pl.ds(0, (sizes[r] - 1) * STRIPS)], send_sem.at[2 + r])
        local_wait(pick[r].at[:, pl.ds(0, sizes[r] - 1)], send_sem.at[5 + r])
    local_wait(label_got.at[pl.ds(0, BAND - 1)], send_sem.at[4])
    local_wait(spread.at[:, pl.ds(0, BAND - 1)], send_sem.at[7])

    local_wait(owned.at[pl.ds(0, devices - 1)], owner_sem)
    for r in range(BAND):
        total = owned[r]
        for k in range(1, devices // BAND):
            total = total + owned[k * BAND + r]
        out[:, r, :] = total
    local_wait(sums.at[pl.ds(0, devices - 1)], send_sem.at[8])


def local(slabs, tiles, fixed, moving, pair_dest, pair_slot, plane_shift, live_count, piece_block):
    table = tables()
    devices = slabs * tiles
    labels = jnp.pad(piece_block.reshape(STRIPS, PIECES), ((0, 8 - STRIPS), (0, W - PIECES)))
    smem = pl.BlockSpec(memory_space=pltpu.SMEM)
    vmem = pl.BlockSpec(memory_space=pltpu.VMEM)
    anywhere = pl.BlockSpec(memory_space=pl.ANY)
    dma = pltpu.SemaphoreType.DMA
    return pl.pallas_call(
        functools.partial(whole_kernel, slabs, tiles),
        out_shape=(
            jax.ShapeDtypeStruct((2, STRIPS), F32),
            jax.ShapeDtypeStruct((OWNED, BAND, W), F32),
        ),
        in_specs=[smem, smem, smem, smem, vmem, anywhere, anywhere, anywhere],
        out_specs=(vmem, vmem),
        scratch_shapes=[
            pltpu.VMEM((STRIPS, H, W), F32),
            pltpu.VMEM((2, TABLE_ROWS, HALF), BF16),
            pltpu.VMEM((slabs * STRIPS, H // slabs, W), F32),
            pltpu.VMEM((tiles * STRIPS, H // tiles, W), F32),
            pltpu.VMEM((STRIPS, slabs, H // slabs, W), F32),
            pltpu.VMEM((STRIPS, tiles, H // tiles, W), F32),
            pltpu.VMEM((2, STRIPS, H, W), F32),
            pltpu.VMEM((slabs, 8, W), jnp.int32),
            pltpu.VMEM((tiles, 8, W), jnp.int32),
            pltpu.VMEM((2, 8, W), jnp.int32),
            pltpu.SMEM((2, 8, W), jnp.int32),
            pltpu.VMEM((STRIPS, SPEC, 2 * W), F32),
            pltpu.VMEM((PIECES * PAD, W), F32),
            pltpu.VMEM((STRIPS, BAND, PIECES, W), F32),
            pltpu.VMEM((STRIPS, BAND, PIECES, W), F32),
            pltpu.VMEM((BAND, 8, W), jnp.int32),
            pltpu.VMEM((STRIPS, devices * OWNED, BAND * PIECES), BF16),
            pltpu.VMEM((devices, OWNED, W), F32),
            pltpu.VMEM((devices, OWNED, W), F32),
            dma((9,)), dma((2,)), dma((2,)), dma, dma((2, STRIPS)), dma((STRIPS,)), dma((5,)), dma,
            pltpu.SemaphoreType.REGULAR,
        ],
        compiler_params=pltpu.CompilerParams(
            collective_id=0, has_side_effects=True, vmem_limit_bytes=60 * 1024 * 1024
        ),
        name="register_merge",
    )(pair_dest, pair_slot, plane_shift, live_count, labels, moving, fixed, table)


def solution(mesh):
    both = ("slab", "tile")
    placed = (
        P(both, None, None),
        P(None, both, None, None),
        P(None, both),
        P(None, both),
        P(None, None, both),
        P(both),
        P(both),
    )
    return jax.shard_map(
        functools.partial(local, mesh.shape["slab"], mesh.shape["tile"]),
        mesh=mesh,
        in_specs=placed,
        out_specs=(P(None, both), P(both, None, None)),
        check_vma=False,
    )
```

```python
import functools
import math

import jax
import jax.numpy as jnp
import ml_dtypes
import numpy as np
from jax import lax
from jax.experimental import pallas as pl
from jax.experimental.pallas import tpu as pltpu
from jax.sharding import PartitionSpec as P

MESH = pl.DeviceIdType.MESH
F32 = jnp.float32
BF16 = jnp.bfloat16
H = 512
W = 128
STRIPS = 4
PIECES = 16
BAND = H // PIECES
OWNED = 16
HALF = H // 2
QUARTER = HALF // 2
SPEC = HALF + 8
PAD = BAND + 8
RING = 4
GROUP = 2 * BAND
HALF_LANES = W // 2
SHARE = PIECES // 2
FIRST = HALF + 16


def tables():
    n = np.arange(HALF)
    even = np.arange(0, HALF, 2)
    odd = np.arange(1, HALF, 2)
    row_scale = 1.0 / math.sqrt(H)

    def cos_rows(k):
        return np.cos(2 * np.pi * ((k[:, None] * n[None, :]) % H) / H) * row_scale

    def sin_rows(k):
        return np.sin(2 * np.pi * ((k[:, None] * n[None, :]) % H) / H) * row_scale

    last = np.zeros((16, HALF))
    last[0] = np.where(n % 2 == 0, 1.0, -1.0) * row_scale
    forward_even = np.concatenate([cos_rows(even), last, -sin_rows(even)], 0)
    forward_odd = np.concatenate([cos_rows(odd), -sin_rows(odd)], 0)
    re_part = 2 * cos_rows(even)
    re_part[0] *= 0.5
    im_part = -2 * sin_rows(even)
    im_part[0] = last[0]
    back_even = np.concatenate([re_part, im_part], 0).T
    back_odd = np.concatenate([2 * cos_rows(odd), -2 * sin_rows(odd)], 0).T
    m = np.arange(W)
    angle = 2 * np.pi * ((m[:, None] * m[None, :]) % W) / W
    c, s = np.cos(angle) / math.sqrt(W), np.sin(angle) / math.sqrt(W)
    column_forward = np.block([[c, -s], [s, c]])
    column_back = np.block([[c, s], [-s, c]])
    table = np.concatenate(
        [forward_even, forward_odd, column_forward, column_back, back_even, back_odd], 0
    )
    high = table.astype(ml_dtypes.bfloat16)
    low = (table - high.astype(np.float64)).astype(ml_dtypes.bfloat16)
    return jnp.asarray(np.stack([high, low]))


TABLE_ROWS = FIRST + 5 * HALF


def dot(a, b):
    return jnp.dot(a, b, preferred_element_type=F32)


def split(x):
    high = x.astype(BF16)
    return high, (x - high.astype(F32)).astype(BF16)


def part(table, index):
    start, rows = (0, FIRST) if index == 0 else (FIRST + HALF * (index - 1), HALF)
    return table[0, start : start + rows, :], table[1, start : start + rows, :]


def left(table, index, x):
    high, low = part(table, index)
    xh, xl = split(x)
    return dot(high, xh) + (dot(low, xh) + dot(high, xl))


def right(x, table, index):
    high, low = part(table, index)
    xh, xl = split(x)
    return dot(xh, high) + (dot(xl, high) + dot(xh, low))


def forward_pair(table, a, b):
    x = jnp.concatenate([a, b], 1)
    u = left(table, 0, x[:HALF] + x[HALF:])
    v = left(table, 1, x[:HALF] - x[HALF:])
    joined = []
    for i in range(2):
        lanes = slice(W * i, W * (i + 1))
        re_part = jnp.concatenate(
            [u[:QUARTER, lanes], v[:QUARTER, lanes], u[QUARTER : QUARTER + 8, lanes]], 0)
        im_part = jnp.concatenate(
            [u[QUARTER + 16 :, lanes], v[QUARTER:, lanes], jnp.zeros((8, W), F32)], 0)
        joined.append(jnp.concatenate([re_part, im_part], 1))
    return right(jnp.concatenate(joined, 0), table, 2)


def surfaces(table, fixed_spectrum, spectra):
    fr, fi = fixed_spectrum[:, :W], fixed_spectrum[:, W:]
    crossed = []
    for i in range(2):
        gr, gi = spectra[SPEC * i : SPEC * (i + 1), :W], spectra[SPEC * i : SPEC * (i + 1), W:]
        cr = fr * gr + fi * gi
        ci = fi * gr - fr * gi
        scale = lax.rsqrt(cr * cr + ci * ci + 0.0625)
        crossed.append(jnp.concatenate([cr * scale, ci * scale], 1))
    back = right(jnp.concatenate(crossed, 0), table, 3)
    evens, odds = [], []
    first = lax.broadcasted_iota(jnp.int32, (8, W), 0) == 0
    for i in range(2):
        pr, pi = back[SPEC * i : SPEC * (i + 1), :W], back[SPEC * i : SPEC * (i + 1), W:]
        evens.append(jnp.concatenate(
            [pr[:QUARTER], jnp.where(first, pr[HALF:], pi[:8]), pi[8:QUARTER]], 0))
        odds.append(jnp.concatenate([pr[QUARTER:HALF], pi[QUARTER:HALF]], 0))
    even = left(table, 4, jnp.concatenate(evens, 1))
    odd = left(table, 5, jnp.concatenate(odds, 1))
    return even + jnp.abs(odd)


def far_first(*sizes):
    grid = [[]]
    for size in sizes:
        grid = [g + [v] for g in grid for v in range(size)]
    grid = [tuple(g) for g in grid if any(g)]

    def hops(g):
        return sum(min(v, RING - v) for v in g[:-1]) + (
            min(g[-1], RING - g[-1]) if sizes[-1] == RING else 0.25 * g[-1])

    return sorted(grid, key=lambda g: (-hops(g), g))


def whole_kernel(
    slabs, tiles, dest_in, slot_in, shifts_in, live, block_in, moving, fixed_in, table_in,
    peaks, owned, dest, slot, shifts, block, fixed, table, got0, got1, pick0, pick1, partner, code0, code1, inv_v, inv_s, fixed_spec,
    merged, spread, rows_got, label_got, onehot, sums, packed,
    send_sem, spread_sem, code_sem, label_sem, slot_sem, rows_sem, own_sem, owner_sem, ready,
):
    p = lax.axis_index("slab")
    q = lax.axis_index("tile")
    z, x = p // RING, lax.rem(p, RING)
    y, c = q // 2, lax.rem(q, 2)
    me = p * tiles + q
    member = lax.rem(me, GROUP)
    devices = slabs * tiles
    axes = ("slab", "tile")
    sizes = (slabs, tiles)
    mine = (p, q)
    got = (got0, got1)
    pick = (pick0, pick1)
    code = (code0, code1)
    rows = (H // slabs, H // tiles)

    def slab_peer(g):
        return lax.rem(z + g[0], RING) * RING + lax.rem(x + g[1], RING)

    def tile_peer(g):
        return lax.rem(y + g[0], RING) * 2 + lax.rem(c + g[1], 2)

    peers = (
        [slab_peer(g) for g in far_first(RING, RING)],
        [tile_peer(g) for g in far_first(RING, 2)],
    )

    def local_wait(ref, sem):
        pltpu.make_async_copy(ref, ref, sem).wait()

    row8 = lax.broadcasted_iota(jnp.int32, (8, W), 0)
    lane8 = lax.broadcasted_iota(jnp.int32, (8, W), 1)

    barrier = pltpu.get_barrier_semaphore()
    for r in range(2):
        for peer in peers[r]:
            pl.semaphore_signal(barrier, inc=1, device_id={axes[r]: peer}, device_id_type=MESH)
    small = [
        pltpu.make_async_copy(a, b, own_sem.at[5 + i])
        for i, (a, b) in enumerate((
            (dest_in, dest), (slot_in, slot), (shifts_in, shifts), (block_in, block)))
    ]
    for copy in small:
        copy.start()
    for copy in small:
        copy.wait()
    for r in range(2):
        tile = jnp.full((8, W), -1, jnp.int32)
        for s in range(STRIPS):
            tile = jnp.where(row8 == s, dest[r, s] * STRIPS + slot[r, s], tile)
        code[r][mine[r]] = tile
    tile = jnp.zeros((8, W), jnp.int32)
    for s in range(STRIPS):
        for k in range(PIECES):
            at = (row8 == (k // SHARE) * STRIPS + s) & (lane8 == k % SHARE)
            tile = jnp.where(at, block[s * PIECES + k], tile)
    label_got[member] = pltpu.roll(tile, lax.rem(member, W // SHARE) * SHARE, 1)
    pl.semaphore_wait(barrier, slabs + tiles - 2)

    for r in range(2):
        for peer in peers[r]:
            pltpu.make_async_remote_copy(
                src_ref=code[r].at[mine[r]], dst_ref=code[r].at[mine[r]],
                send_sem=send_sem.at[r], recv_sem=code_sem.at[r],
                device_id={axes[r]: peer}, device_id_type=MESH,
            ).start()

    def spread_start(r, i):
        peer = peers[r][i]
        pltpu.make_async_remote_copy(
            src_ref=moving.at[r, :, pl.ds(pl.multiple_of(peer * rows[r], rows[r]), rows[r]), :],
            dst_ref=got[r].at[pl.ds(mine[r] * STRIPS, STRIPS)],
            send_sem=send_sem.at[2 + r], recv_sem=spread_sem.at[r],
            device_id={axes[r]: peer}, device_id_type=MESH,
        ).start()

    for i in range(slabs - 1):
        spread_start(0, i)
        if i % 2 == 0 and i // 2 < tiles - 1:
            spread_start(1, i // 2)
    own = [
        pltpu.make_async_copy(
            moving.at[r, :, pl.ds(pl.multiple_of(mine[r] * rows[r], rows[r]), rows[r]), :],
            got[r].at[pl.ds(mine[r] * STRIPS, STRIPS)], own_sem.at[r])
        for r in range(2)
    ]
    load_fixed = pltpu.make_async_copy(fixed_in, fixed, own_sem.at[2])
    load_table = pltpu.make_async_copy(table_in, table, own_sem.at[3])
    load_fixed.start()
    load_table.start()
    for copy in own:
        copy.start()
    for peer in peers[0]:
        pl.semaphore_signal(ready, inc=1, device_id={"slab": peer}, device_id_type=MESH)

    for r in range(2):
        local_wait(code[r].at[pl.ds(0, sizes[r] - 1)], code_sem.at[r])
        total = jnp.zeros((8, W), jnp.int32)
        for i in range(sizes[r]):
            total += jnp.where(code[r][i] == lane8, i * STRIPS + row8, 0)
        source = jnp.minimum(jnp.sum(total, 0, keepdims=True), sizes[r] * STRIPS - 1)
        inv_v[r] = jnp.broadcast_to(source, (8, W))
    to_scalars = pltpu.make_async_copy(inv_v, inv_s, own_sem.at[4])
    to_scalars.start()

    pl.semaphore_wait(ready, slabs - 1)
    group_base = (p // (GROUP // tiles)) * (GROUP // tiles)

    def group_peer(step):
        peer = lax.rem(member + step, GROUP)
        return peer, (group_base + peer // tiles, lax.rem(peer, tiles))

    def send_label(step, carry):
        pltpu.make_async_remote_copy(
            src_ref=label_got.at[member], dst_ref=label_got.at[member],
            send_sem=send_sem.at[4], recv_sem=label_sem,
            device_id=group_peer(step)[1], device_id_type=MESH,
        ).start()
        return carry

    lax.fori_loop(1, GROUP, send_label, 0)

    load_fixed.wait()
    load_table.wait()

    def fixed_pair(i, carry):
        spectra = forward_pair(table, fixed[2 * i], fixed[2 * i + 1])
        fixed_spec[2 * i] = spectra[:SPEC]
        fixed_spec[2 * i + 1] = spectra[SPEC:]
        return carry

    lax.fori_loop(0, STRIPS // 2, fixed_pair, 0)

    local_wait(label_got.at[pl.ds(0, GROUP - 1)], label_sem)
    columns = []
    for g in range(GROUP * SHARE // W):
        total = label_got[W // SHARE * g]
        for d in range(1, W // SHARE):
            total = total + label_got[W // SHARE * g + d]
        columns.append(total)
    chunk = 256

    def build_slot(s):
        def build(i, carry):
            want = lax.broadcasted_iota(jnp.int32, (chunk, W), 0) + i * chunk
            for half in range(2):
                for g, column in enumerate(columns):
                    at = half * STRIPS + s
                    hit = jnp.broadcast_to(column[at : at + 1], (chunk, W)) == want
                    lanes = W * (len(columns) * half + g)
                    onehot[s, pl.ds(pl.multiple_of(i * chunk, chunk), chunk), lanes : lanes + W] = (
                        jnp.where(hit, 1.0, 0.0).astype(BF16))
            return carry

        lax.fori_loop(0, devices * OWNED // chunk, build, 0)

    build_slot(0)
    build_slot(1)

    to_scalars.wait()
    for r in (1, 0):
        own[r].wait()
        local_wait(got[r].at[pl.ds(0, (sizes[r] - 1) * STRIPS)], spread_sem.at[r])

    def choose(s, carry):
        for r in (0, 1):
            place = pl.ds(pl.multiple_of(mine[r] * rows[r], rows[r]), rows[r])
            partner[r, s, place, :] = got[r][inv_s[r, 0, mine[r] * STRIPS + s]]
            for peer in peers[r]:
                pick[r][s, peer] = got[r][inv_s[r, 0, peer * STRIPS + s]]
        for r in (0, 1):
            place = pl.ds(pl.multiple_of(mine[r] * rows[r], rows[r]), rows[r])
            for peer in peers[r]:
                pltpu.make_async_remote_copy(
                    src_ref=pick[r].at[s, peer], dst_ref=partner.at[r, s, place, :],
                    send_sem=send_sem.at[5 + r], recv_sem=slot_sem.at[r, s],
                    device_id={axes[r]: peer}, device_id_type=MESH,
                ).start()
        return carry

    lax.fori_loop(0, STRIPS, choose, 0)

    build_slot(2)
    build_slot(3)

    low_half = lane8 < HALF_LANES

    def correlate(s, found):
        for r in range(2):
            local_wait(partner.at[r, s, pl.ds(0, H - rows[r])], slot_sem.at[r, s])
        spectra = forward_pair(table, partner[0, s], partner[1, s])
        surface = surfaces(table, fixed_spec[s], spectra)
        is_live = s < live[0]
        total = jnp.ones((1, 1), F32)
        acc = fixed[s]
        for r in range(2):
            peak = jnp.max(surface[:, W * r : W * (r + 1)], axis=(0, 1), keepdims=True)
            weight = 1.0 / (1.0 + jnp.exp(4.0 - peak))
            down = lax.rem(shifts[r, 0, s] + H, H)
            side = lax.rem(shifts[r, 1, s] + W, W)
            moved = pltpu.roll(pltpu.roll(partner[r, s], side, 1), down, 0)
            acc = acc + weight * moved
            total = total + weight
            shown = jnp.where(is_live, peak, 0.0)
            found = jnp.where((row8 == r) & (lane8 == s), shown, found)
        acc = jnp.where(is_live, acc * (1.0 / total), 0.0)
        for k in range(PIECES):
            merged[pl.ds(k * PAD, BAND), :] = acc[k * BAND : (k + 1) * BAND]
        for r in range(BAND):
            top = merged[pl.ds(r, SHARE, stride=PAD), :]
            bottom = merged[pl.ds(r + SHARE * PAD, SHARE, stride=PAD), :]
            spread[s, 2 * r] = jnp.where(low_half, top, pltpu.roll(bottom, HALF_LANES, 1))
            spread[s, 2 * r + 1] = jnp.where(low_half, pltpu.roll(top, HALF_LANES, 1), bottom)
        rows_got[s, member] = spread[s, member]

        def send_rows(step, carry):
            peer, device = group_peer(step)
            pltpu.make_async_remote_copy(
                src_ref=spread.at[s, peer], dst_ref=rows_got.at[s, member],
                send_sem=send_sem.at[7], recv_sem=rows_sem.at[s],
                device_id=device, device_id_type=MESH,
            ).start()
            return carry

        lax.fori_loop(1, GROUP, send_rows, 0)
        return found

    found = lax.fori_loop(0, STRIPS, correlate, jnp.zeros((8, W), F32))
    peaks[...] = found

    big = 1024
    low_rows = lax.broadcasted_iota(jnp.int32, (GROUP * SHARE, W), 1) < HALF_LANES
    for s in range(STRIPS):
        local_wait(rows_got.at[s, pl.ds(0, GROUP - 1)], rows_sem.at[s])
        rows_here = rows_got[s].reshape(GROUP * SHARE, W)
        high = rows_here.astype(BF16).astype(F32)
        low = rows_here - high
        both = jnp.concatenate([
            jnp.where(low_rows, high, pltpu.roll(low, HALF_LANES, 1)),
            jnp.where(low_rows, pltpu.roll(high, HALF_LANES, 1), low),
        ], 0).astype(BF16)

        def add(i, carry):
            at = pl.ds(pl.multiple_of(i * big, big), big)
            total = dot(onehot[s, at, :], both)
            if s > 0:
                total = total + sums[at, :]
            if s < STRIPS - 1:
                sums[at, :] = total
            else:
                total = (total + pltpu.roll(total, HALF_LANES, 1)).reshape(big // OWNED, 2, 8, W)
                owners = pl.ds(i * (big // OWNED), big // OWNED)
                packed[owners] = jnp.where(low_half[None], total[:, 0], total[:, 1])
            return carry

        lax.fori_loop(0, devices * OWNED // big, add, 0)

    def send_owner(k, carry):
        oz = lax.rem(z + 2 + k // 32, RING)
        ox = lax.rem(x + 2 + lax.rem(k // 8, RING), RING)
        oy = lax.rem(y + 2 + lax.rem(k // 2, RING), RING)
        oc = lax.rem(c + lax.rem(k, 2), 2)
        op, oq = oz * RING + ox, oy * 2 + oc
        pltpu.make_async_remote_copy(
            src_ref=packed.at[op * tiles + oq], dst_ref=owned.at[me],
            send_sem=send_sem.at[8], recv_sem=owner_sem,
            device_id=(op, oq), device_id_type=MESH,
        ).start()
        return carry

    self_at = 2 * 32 + 2 * 8 + 2 * 2
    lax.fori_loop(0, self_at, send_owner, 0)
    lax.fori_loop(self_at + 1, devices, send_owner, 0)
    last = pltpu.make_async_copy(packed.at[me], owned.at[me], own_sem.at[4])
    last.start()

    for r in range(2):
        local_wait(code[r].at[pl.ds(0, sizes[r] - 1)], send_sem.at[r])
        local_wait(got[r].at[pl.ds(0, (sizes[r] - 1) * STRIPS)], send_sem.at[2 + r])
        local_wait(pick[r].at[:, pl.ds(0, sizes[r] - 1)], send_sem.at[5 + r])
    local_wait(label_got.at[pl.ds(0, GROUP - 1)], send_sem.at[4])
    local_wait(spread.at[:, pl.ds(0, GROUP - 1)], send_sem.at[7])

    last.wait()
    local_wait(packed.at[pl.ds(0, devices - 1)], owner_sem)
    local_wait(packed.at[pl.ds(0, devices - 1)], send_sem.at[8])


def finish_kernel(found, owned, peaks, out):
    peaks[...] = found[:2, :STRIPS]
    low_half = lax.broadcasted_iota(jnp.int32, (8, W), 1) < HALF_LANES
    for r in range(BAND):
        a, b = owned[2 * r], owned[2 * r + 1]
        for k in range(1, owned.shape[0] // GROUP):
            a = a + owned[k * GROUP + 2 * r]
            b = b + owned[k * GROUP + 2 * r + 1]
        out[:8, r, :] = jnp.where(low_half, a, pltpu.roll(b, HALF_LANES, 1))
        out[8:, r, :] = jnp.where(low_half, pltpu.roll(a, HALF_LANES, 1), b)


def local(slabs, tiles, fixed, moving, pair_dest, pair_slot, plane_shift, live_count, piece_block):
    table = tables()
    devices = slabs * tiles
    vmem = pl.BlockSpec(memory_space=pltpu.VMEM)
    anywhere = pl.BlockSpec(memory_space=pl.ANY)
    dma = pltpu.SemaphoreType.DMA
    small = (pair_dest, pair_slot, plane_shift, live_count, piece_block)
    found, owned = pl.pallas_call(
        functools.partial(whole_kernel, slabs, tiles),
        out_shape=(
            jax.ShapeDtypeStruct((8, W), F32),
            jax.ShapeDtypeStruct((devices, 8, W), F32),
        ),
        in_specs=[anywhere] * 3 + [pl.BlockSpec(memory_space=pltpu.SMEM)] + [anywhere] * 4,
        out_specs=(vmem, anywhere),
        scratch_shapes=[pltpu.SMEM(a.shape, jnp.int32) for a in small if a.shape != (1,)]
        + [
            pltpu.VMEM((STRIPS, H, W), F32),
            pltpu.VMEM((2, TABLE_ROWS, HALF), BF16),
            pltpu.VMEM((slabs * STRIPS, H // slabs, W), F32),
            pltpu.VMEM((tiles * STRIPS, H // tiles, W), F32),
            pltpu.VMEM((STRIPS, slabs, H // slabs, W), F32),
            pltpu.VMEM((STRIPS, tiles, H // tiles, W), F32),
            pltpu.VMEM((2, STRIPS, H, W), F32),
            pltpu.VMEM((slabs, 8, W), jnp.int32),
            pltpu.VMEM((tiles, 8, W), jnp.int32),
            pltpu.VMEM((2, 8, W), jnp.int32),
            pltpu.SMEM((2, 8, W), jnp.int32),
            pltpu.VMEM((STRIPS, SPEC, 2 * W), F32),
            pltpu.VMEM((PIECES * PAD, W), F32),
            pltpu.VMEM((STRIPS, GROUP, SHARE, W), F32),
            pltpu.VMEM((STRIPS, GROUP, SHARE, W), F32),
            pltpu.VMEM((GROUP, 8, W), jnp.int32),
            pltpu.VMEM((STRIPS, devices * OWNED, GROUP * PIECES), BF16),
            pltpu.VMEM((devices * OWNED, W), F32),
            pltpu.VMEM((devices, 8, W), F32),
            dma((9,)), dma((2,)), dma((2,)), dma, dma((2, STRIPS)), dma((STRIPS,)), dma((10,)), dma,
            pltpu.SemaphoreType.REGULAR,
        ],
        compiler_params=pltpu.CompilerParams(
            collective_id=0, has_side_effects=True, vmem_limit_bytes=60 * 1024 * 1024
        ),
        name="register_merge",
    )(*small, moving, fixed, table)
    return pl.pallas_call(
        finish_kernel,
        out_shape=(
            jax.ShapeDtypeStruct((2, STRIPS), F32),
            jax.ShapeDtypeStruct((OWNED, BAND, W), F32),
        ),
        in_specs=[vmem, vmem],
        out_specs=(vmem, vmem),
        name="finish_blocks",
    )(found, owned)


def solution(mesh):
    both = ("slab", "tile")
    placed = (
        P(both, None, None),
        P(None, both, None, None),
        P(None, both),
        P(None, both),
        P(None, None, both),
        P(both),
        P(both),
    )
    return jax.shard_map(
        functools.partial(local, mesh.shape["slab"], mesh.shape["tile"]),
        mesh=mesh,
        in_specs=placed,
        out_specs=(P(None, both), P(both, None, None)),
        check_vma=False,
    )
```

```python
import functools
import math

import jax
import jax.numpy as jnp
import ml_dtypes
import numpy as np
from jax import lax
from jax.experimental import pallas as pl
from jax.experimental.pallas import tpu as pltpu
from jax.sharding import PartitionSpec as P

MESH = pl.DeviceIdType.MESH
F32 = jnp.float32
BF16 = jnp.bfloat16
H = 512
W = 128
STRIPS = 4
PIECES = 16
BAND = H // PIECES
OWNED = 16
HALF = H // 2
QUARTER = HALF // 2
SPEC = HALF + 8
PAD = BAND + 8
RING = 4
GROUP = 2 * BAND
HALF_LANES = W // 2
SHARE = PIECES // 2
FIRST = HALF + 16


def tables():
    n = np.arange(HALF)
    even = np.arange(0, HALF, 2)
    odd = np.arange(1, HALF, 2)
    row_scale = 1.0 / math.sqrt(H)

    def cos_rows(k):
        return np.cos(2 * np.pi * ((k[:, None] * n[None, :]) % H) / H) * row_scale

    def sin_rows(k):
        return np.sin(2 * np.pi * ((k[:, None] * n[None, :]) % H) / H) * row_scale

    last = np.zeros((16, HALF))
    last[0] = np.where(n % 2 == 0, 1.0, -1.0) * row_scale
    forward_even = np.concatenate([cos_rows(even), last, -sin_rows(even)], 0)
    forward_odd = np.concatenate([cos_rows(odd), -sin_rows(odd)], 0)
    re_part = 2 * cos_rows(even)
    re_part[0] *= 0.5
    im_part = -2 * sin_rows(even)
    im_part[0] = last[0]
    back_even = np.concatenate([re_part, im_part], 0).T
    back_odd = np.concatenate([2 * cos_rows(odd), -2 * sin_rows(odd)], 0).T
    m = np.arange(W)
    angle = 2 * np.pi * ((m[:, None] * m[None, :]) % W) / W
    c, s = np.cos(angle) / math.sqrt(W), np.sin(angle) / math.sqrt(W)
    column_forward = np.block([[c, -s], [s, c]])
    column_back = np.block([[c, s], [-s, c]])
    table = np.concatenate(
        [forward_even, forward_odd, column_forward, column_back, back_even, back_odd], 0
    )
    high = table.astype(ml_dtypes.bfloat16)
    low = (table - high.astype(np.float64)).astype(ml_dtypes.bfloat16)
    return jnp.asarray(np.stack([high, low]))


TABLE_ROWS = FIRST + 5 * HALF


def dot(a, b):
    return jnp.dot(a, b, preferred_element_type=F32)


def split(x):
    high = x.astype(BF16)
    return high, (x - high.astype(F32)).astype(BF16)


def part(table, index):
    start, rows = (0, FIRST) if index == 0 else (FIRST + HALF * (index - 1), HALF)
    return table[0, start : start + rows, :], table[1, start : start + rows, :]


def left(table, index, x):
    high, low = part(table, index)
    xh, xl = split(x)
    return dot(high, xh) + (dot(low, xh) + dot(high, xl))


def right(x, table, index):
    high, low = part(table, index)
    xh, xl = split(x)
    return dot(xh, high) + (dot(xl, high) + dot(xh, low))


def forward_pair(table, a, b):
    x = jnp.concatenate([a, b], 1)
    u = left(table, 0, x[:HALF] + x[HALF:])
    v = left(table, 1, x[:HALF] - x[HALF:])
    joined = []
    for i in range(2):
        lanes = slice(W * i, W * (i + 1))
        re_part = jnp.concatenate(
            [u[:QUARTER, lanes], v[:QUARTER, lanes], u[QUARTER : QUARTER + 8, lanes]], 0)
        im_part = jnp.concatenate(
            [u[QUARTER + 16 :, lanes], v[QUARTER:, lanes], jnp.zeros((8, W), F32)], 0)
        joined.append(jnp.concatenate([re_part, im_part], 1))
    return right(jnp.concatenate(joined, 0), table, 2)


def surfaces(table, fixed_spectrum, spectra):
    fr, fi = fixed_spectrum[:, :W], fixed_spectrum[:, W:]
    crossed = []
    for i in range(2):
        gr, gi = spectra[SPEC * i : SPEC * (i + 1), :W], spectra[SPEC * i : SPEC * (i + 1), W:]
        cr = fr * gr + fi * gi
        ci = fi * gr - fr * gi
        scale = lax.rsqrt(cr * cr + ci * ci + 0.0625)
        crossed.append(jnp.concatenate([cr * scale, ci * scale], 1))
    back = right(jnp.concatenate(crossed, 0), table, 3)
    evens, odds = [], []
    first = lax.broadcasted_iota(jnp.int32, (8, W), 0) == 0
    for i in range(2):
        pr, pi = back[SPEC * i : SPEC * (i + 1), :W], back[SPEC * i : SPEC * (i + 1), W:]
        evens.append(jnp.concatenate(
            [pr[:QUARTER], jnp.where(first, pr[HALF:], pi[:8]), pi[8:QUARTER]], 0))
        odds.append(jnp.concatenate([pr[QUARTER:HALF], pi[QUARTER:HALF]], 0))
    even = left(table, 4, jnp.concatenate(evens, 1))
    odd = left(table, 5, jnp.concatenate(odds, 1))
    return even + jnp.abs(odd)


def far_first(*sizes):
    grid = [[]]
    for size in sizes:
        grid = [g + [v] for g in grid for v in range(size)]
    grid = [tuple(g) for g in grid if any(g)]

    def hops(g):
        return sum(min(v, RING - v) for v in g[:-1]) + (
            min(g[-1], RING - g[-1]) if sizes[-1] == RING else 0.25 * g[-1])

    return sorted(grid, key=lambda g: (-hops(g), g))


def whole_kernel(
    slabs, tiles, dest_in, slot_in, shifts_in, live, block_in, moving, fixed_in, table_in,
    peaks, owned, dest, slot, shifts, block, fixed, table, got00, got01, got10, got11, pick0, pick1, partner, code0, code1, inv_v, inv_s, fixed_spec,
    merged, spread, rows_got, label_got, onehot, sums, packed,
    send_sem, spread_sem, code_sem, label_sem, slot_sem, rows_sem, own_sem, owner_sem, ready,
):
    p = lax.axis_index("slab")
    q = lax.axis_index("tile")
    z, x = p // RING, lax.rem(p, RING)
    y, c = q // 2, lax.rem(q, 2)
    me = p * tiles + q
    member = lax.rem(me, GROUP)
    devices = slabs * tiles
    axes = ("slab", "tile")
    sizes = (slabs, tiles)
    mine = (p, q)
    got = ((got00, got01), (got10, got11))
    pick = (pick0, pick1)
    code = (code0, code1)
    rows = (H // slabs, H // tiles)

    def slab_peer(g):
        return lax.rem(z + g[0], RING) * RING + lax.rem(x + g[1], RING)

    def tile_peer(g):
        return lax.rem(y + g[0], RING) * 2 + lax.rem(c + g[1], 2)

    peers = (
        [slab_peer(g) for g in far_first(RING, RING)],
        [tile_peer(g) for g in far_first(RING, 2)],
    )

    def local_wait(ref, sem):
        pltpu.make_async_copy(ref, ref, sem).wait()

    row8 = lax.broadcasted_iota(jnp.int32, (8, W), 0)
    lane8 = lax.broadcasted_iota(jnp.int32, (8, W), 1)

    barrier = pltpu.get_barrier_semaphore()
    for r in range(2):
        for peer in peers[r]:
            pl.semaphore_signal(barrier, inc=1, device_id={axes[r]: peer}, device_id_type=MESH)
    small = [
        pltpu.make_async_copy(a, b, own_sem.at[5 + i])
        for i, (a, b) in enumerate((
            (dest_in, dest), (slot_in, slot), (shifts_in, shifts), (block_in, block)))
    ]
    for copy in small:
        copy.start()
    for copy in small:
        copy.wait()
    for r in range(2):
        tile = jnp.full((8, W), -1, jnp.int32)
        for s in range(STRIPS):
            tile = jnp.where(row8 == s, dest[r, s] * STRIPS + slot[r, s], tile)
        code[r][mine[r]] = tile
    tile = jnp.zeros((8, W), jnp.int32)
    for s in range(STRIPS):
        for k in range(PIECES):
            at = (row8 == (k // SHARE) * STRIPS + s) & (lane8 == k % SHARE)
            tile = jnp.where(at, block[s * PIECES + k], tile)
    label_got[member] = pltpu.roll(tile, lax.rem(member, W // SHARE) * SHARE, 1)
    pl.semaphore_wait(barrier, slabs + tiles - 2)

    for r in range(2):
        for peer in peers[r]:
            pltpu.make_async_remote_copy(
                src_ref=code[r].at[mine[r]], dst_ref=code[r].at[mine[r]],
                send_sem=send_sem.at[r], recv_sem=code_sem.at[r],
                device_id={axes[r]: peer}, device_id_type=MESH,
            ).start()

    def chunk_rows(r, at, half):
        part_rows = rows[r] // 2
        return pl.ds(pl.multiple_of(at * rows[r] + half * part_rows, part_rows), part_rows)

    def spread_start(r, i, half):
        peer = peers[r][i]
        pltpu.make_async_remote_copy(
            src_ref=moving.at[r, :, chunk_rows(r, peer, half), :],
            dst_ref=got[r][half].at[pl.ds(mine[r] * STRIPS, STRIPS)],
            send_sem=send_sem.at[2 + r], recv_sem=spread_sem.at[r, half],
            device_id={axes[r]: peer}, device_id_type=MESH,
        ).start()

    own = []
    for half in range(2):
        for i in range(slabs - 1):
            spread_start(0, i, half)
            if i % 2 == 0 and i // 2 < tiles - 1:
                spread_start(1, i // 2, half)
        own.append([
            pltpu.make_async_copy(
                moving.at[r, :, chunk_rows(r, mine[r], half), :],
                got[r][half].at[pl.ds(mine[r] * STRIPS, STRIPS)], own_sem.at[2 * r + half])
            for r in range(2)
        ])
    load_fixed = pltpu.make_async_copy(fixed_in, fixed, own_sem.at[10])
    load_table = pltpu.make_async_copy(table_in, table, own_sem.at[11])
    load_fixed.start()
    load_table.start()
    for copy in own[0] + own[1]:
        copy.start()
    for peer in peers[0]:
        pl.semaphore_signal(ready, inc=1, device_id={"slab": peer}, device_id_type=MESH)

    for r in range(2):
        local_wait(code[r].at[pl.ds(0, sizes[r] - 1)], code_sem.at[r])
        total = jnp.zeros((8, W), jnp.int32)
        for i in range(sizes[r]):
            total += jnp.where(code[r][i] == lane8, i * STRIPS + row8, 0)
        source = jnp.minimum(jnp.sum(total, 0, keepdims=True), sizes[r] * STRIPS - 1)
        inv_v[r] = jnp.broadcast_to(source, (8, W))
    to_scalars = pltpu.make_async_copy(inv_v, inv_s, own_sem.at[4])
    to_scalars.start()

    pl.semaphore_wait(ready, slabs - 1)
    group_rows = GROUP // tiles
    group_base = (p // group_rows) * group_rows
    tile_ring = [lax.rem(q + i, tiles) for i in range(tiles)]

    def to_group(send):
        for i in range(1, tiles):
            send(member - q + tile_ring[i], (p, tile_ring[i]))

        def row(j, carry):
            at = lax.rem(p + j, group_rows)
            for i in range(tiles):
                send(at * tiles + tile_ring[i], (group_base + at, tile_ring[i]))
            return carry

        lax.fori_loop(1, group_rows, row, 0)

    def send_label(peer, device):
        pltpu.make_async_remote_copy(
            src_ref=label_got.at[member], dst_ref=label_got.at[member],
            send_sem=send_sem.at[4], recv_sem=label_sem,
            device_id=device, device_id_type=MESH,
        ).start()

    to_group(send_label)

    load_fixed.wait()
    load_table.wait()

    def fixed_pair(i, carry):
        spectra = forward_pair(table, fixed[2 * i], fixed[2 * i + 1])
        fixed_spec[2 * i] = spectra[:SPEC]
        fixed_spec[2 * i + 1] = spectra[SPEC:]
        return carry

    lax.fori_loop(0, STRIPS // 2, fixed_pair, 0)

    local_wait(label_got.at[pl.ds(0, GROUP - 1)], label_sem)
    columns = []
    for g in range(GROUP * SHARE // W):
        total = label_got[W // SHARE * g]
        for d in range(1, W // SHARE):
            total = total + label_got[W // SHARE * g + d]
        columns.append(total)
    chunk = 256

    def build_slot(s):
        def build(i, carry):
            want = lax.broadcasted_iota(jnp.int32, (chunk, W), 0) + i * chunk
            for half in range(2):
                for g, column in enumerate(columns):
                    at = half * STRIPS + s
                    hit = jnp.broadcast_to(column[at : at + 1], (chunk, W)) == want
                    lanes = W * (len(columns) * half + g)
                    onehot[s, pl.ds(pl.multiple_of(i * chunk, chunk), chunk), lanes : lanes + W] = (
                        jnp.where(hit, 1.0, 0.0).astype(BF16))
            return carry

        lax.fori_loop(0, devices * OWNED // chunk, build, 0)

    build_slot(0)
    build_slot(1)

    to_scalars.wait()

    def second(half):
        for r in (1, 0):
            own[half][r].wait()
            local_wait(got[r][half].at[pl.ds(0, (sizes[r] - 1) * STRIPS)], spread_sem.at[r, half])

        def choose(s, carry):
            for r in (0, 1):
                place = chunk_rows(r, mine[r], half)
                partner[r, s, place, :] = got[r][half][inv_s[r, 0, mine[r] * STRIPS + s]]
                for peer in peers[r]:
                    pick[r][half, s, peer] = got[r][half][inv_s[r, 0, peer * STRIPS + s]]
            for r in (0, 1):
                place = chunk_rows(r, mine[r], half)
                for peer in peers[r]:
                    pltpu.make_async_remote_copy(
                        src_ref=pick[r].at[half, s, peer], dst_ref=partner.at[r, s, place, :],
                        send_sem=send_sem.at[5 + r], recv_sem=slot_sem.at[r, s],
                        device_id={axes[r]: peer}, device_id_type=MESH,
                    ).start()
            return carry

        lax.fori_loop(0, STRIPS, choose, 0)

    second(0)
    build_slot(2)
    build_slot(3)
    second(1)

    low_half = lane8 < HALF_LANES

    def correlate(s, found):
        for r in range(2):
            local_wait(partner.at[r, s, pl.ds(0, H - rows[r])], slot_sem.at[r, s])
        spectra = forward_pair(table, partner[0, s], partner[1, s])
        surface = surfaces(table, fixed_spec[s], spectra)
        is_live = s < live[0]
        total = jnp.ones((1, 1), F32)
        acc = fixed[s]
        for r in range(2):
            peak = jnp.max(surface[:, W * r : W * (r + 1)], axis=(0, 1), keepdims=True)
            weight = 1.0 / (1.0 + jnp.exp(4.0 - peak))
            down = lax.rem(shifts[r, 0, s] + H, H)
            side = lax.rem(shifts[r, 1, s] + W, W)
            moved = pltpu.roll(pltpu.roll(partner[r, s], side, 1), down, 0)
            acc = acc + weight * moved
            total = total + weight
            shown = jnp.where(is_live, peak, 0.0)
            found = jnp.where((row8 == r) & (lane8 == s), shown, found)
        acc = jnp.where(is_live, acc * (1.0 / total), 0.0)
        for k in range(PIECES):
            merged[pl.ds(k * PAD, BAND), :] = acc[k * BAND : (k + 1) * BAND]
        for r in range(BAND):
            top = merged[pl.ds(r, SHARE, stride=PAD), :]
            bottom = merged[pl.ds(r + SHARE * PAD, SHARE, stride=PAD), :]
            spread[s, 2 * r] = jnp.where(low_half, top, pltpu.roll(bottom, HALF_LANES, 1))
            spread[s, 2 * r + 1] = jnp.where(low_half, pltpu.roll(top, HALF_LANES, 1), bottom)
        rows_got[s, member] = spread[s, member]

        def send_rows(peer, device):
            pltpu.make_async_remote_copy(
                src_ref=spread.at[s, peer], dst_ref=rows_got.at[s, member],
                send_sem=send_sem.at[7], recv_sem=rows_sem.at[s],
                device_id=device, device_id_type=MESH,
            ).start()

        to_group(send_rows)
        return found

    found = lax.fori_loop(0, STRIPS, correlate, jnp.zeros((8, W), F32))
    peaks[...] = found

    big = 1024
    low_rows = lax.broadcasted_iota(jnp.int32, (GROUP * SHARE, W), 1) < HALF_LANES
    for s in range(STRIPS):
        local_wait(rows_got.at[s, pl.ds(0, GROUP - 1)], rows_sem.at[s])
        rows_here = rows_got[s].reshape(GROUP * SHARE, W)
        high = rows_here.astype(BF16).astype(F32)
        low = rows_here - high
        both = jnp.concatenate([
            jnp.where(low_rows, high, pltpu.roll(low, HALF_LANES, 1)),
            jnp.where(low_rows, pltpu.roll(high, HALF_LANES, 1), low),
        ], 0).astype(BF16)

        def add(i, carry):
            at = pl.ds(pl.multiple_of(i * big, big), big)
            total = dot(onehot[s, at, :], both)
            if s > 0:
                total = total + sums[at, :]
            if s < STRIPS - 1:
                sums[at, :] = total
            else:
                total = (total + pltpu.roll(total, HALF_LANES, 1)).reshape(big // OWNED, 2, 8, W)
                owners = pl.ds(i * (big // OWNED), big // OWNED)
                packed[owners] = jnp.where(low_half[None], total[:, 0], total[:, 1])
            return carry

        lax.fori_loop(0, devices * OWNED // big, add, 0)

    def send_owner(op, oq):
        pltpu.make_async_remote_copy(
            src_ref=packed.at[op * tiles + oq], dst_ref=owned.at[me],
            send_sem=send_sem.at[8], recv_sem=owner_sem,
            device_id=(op, oq), device_id_type=MESH,
        ).start()

    def owner_row(j, carry):
        op = lax.rem(z + 2 + j // RING, RING) * RING + lax.rem(x + 2 + lax.rem(j, RING), RING)
        for oq in peers[1] + [q]:
            send_owner(op, oq)
        return carry

    own_row = 2 * RING + 2
    lax.fori_loop(0, own_row, owner_row, 0)
    for oq in peers[1]:
        send_owner(p, oq)
    lax.fori_loop(own_row + 1, slabs, owner_row, 0)
    last = pltpu.make_async_copy(packed.at[me], owned.at[me], own_sem.at[4])
    last.start()

    for r in range(2):
        local_wait(code[r].at[pl.ds(0, sizes[r] - 1)], send_sem.at[r])
        local_wait(pick[r].at[:, :, pl.ds(0, sizes[r] - 1)], send_sem.at[2 + r])
        local_wait(pick[r].at[:, :, pl.ds(0, sizes[r] - 1)], send_sem.at[5 + r])
    local_wait(label_got.at[pl.ds(0, GROUP - 1)], send_sem.at[4])
    local_wait(spread.at[:, pl.ds(0, GROUP - 1)], send_sem.at[7])

    last.wait()
    local_wait(packed.at[pl.ds(0, devices - 1)], owner_sem)
    local_wait(packed.at[pl.ds(0, devices - 1)], send_sem.at[8])


def finish_kernel(found, owned, peaks, out):
    peaks[...] = found[:2, :STRIPS]
    low_half = lax.broadcasted_iota(jnp.int32, (8, W), 1) < HALF_LANES
    for r in range(BAND):
        a, b = owned[2 * r], owned[2 * r + 1]
        for k in range(1, owned.shape[0] // GROUP):
            a = a + owned[k * GROUP + 2 * r]
            b = b + owned[k * GROUP + 2 * r + 1]
        out[:8, r, :] = jnp.where(low_half, a, pltpu.roll(b, HALF_LANES, 1))
        out[8:, r, :] = jnp.where(low_half, pltpu.roll(a, HALF_LANES, 1), b)


def local(slabs, tiles, fixed, moving, pair_dest, pair_slot, plane_shift, live_count, piece_block):
    table = tables()
    devices = slabs * tiles
    vmem = pl.BlockSpec(memory_space=pltpu.VMEM)
    anywhere = pl.BlockSpec(memory_space=pl.ANY)
    dma = pltpu.SemaphoreType.DMA
    small = (pair_dest, pair_slot, plane_shift, live_count, piece_block)
    found, owned = pl.pallas_call(
        functools.partial(whole_kernel, slabs, tiles),
        out_shape=(
            jax.ShapeDtypeStruct((8, W), F32),
            jax.ShapeDtypeStruct((devices, 8, W), F32),
        ),
        in_specs=[anywhere] * 3 + [pl.BlockSpec(memory_space=pltpu.SMEM)] + [anywhere] * 4,
        out_specs=(vmem, anywhere),
        scratch_shapes=[pltpu.SMEM(a.shape, jnp.int32) for a in small if a.shape != (1,)]
        + [
            pltpu.VMEM((STRIPS, H, W), F32),
            pltpu.VMEM((2, TABLE_ROWS, HALF), BF16),
            pltpu.VMEM((slabs * STRIPS, H // slabs // 2, W), F32),
            pltpu.VMEM((slabs * STRIPS, H // slabs // 2, W), F32),
            pltpu.VMEM((tiles * STRIPS, H // tiles // 2, W), F32),
            pltpu.VMEM((tiles * STRIPS, H // tiles // 2, W), F32),
            pltpu.VMEM((2, STRIPS, slabs, H // slabs // 2, W), F32),
            pltpu.VMEM((2, STRIPS, tiles, H // tiles // 2, W), F32),
            pltpu.VMEM((2, STRIPS, H, W), F32),
            pltpu.VMEM((slabs, 8, W), jnp.int32),
            pltpu.VMEM((tiles, 8, W), jnp.int32),
            pltpu.VMEM((2, 8, W), jnp.int32),
            pltpu.SMEM((2, 8, W), jnp.int32),
            pltpu.VMEM((STRIPS, SPEC, 2 * W), F32),
            pltpu.VMEM((PIECES * PAD, W), F32),
            pltpu.VMEM((STRIPS, GROUP, SHARE, W), F32),
            pltpu.VMEM((STRIPS, GROUP, SHARE, W), F32),
            pltpu.VMEM((GROUP, 8, W), jnp.int32),
            pltpu.VMEM((STRIPS, devices * OWNED, GROUP * PIECES), BF16),
            pltpu.VMEM((devices * OWNED, W), F32),
            pltpu.VMEM((devices, 8, W), F32),
            dma((9,)), dma((2, 2)), dma((2,)), dma, dma((2, STRIPS)), dma((STRIPS,)), dma((12,)), dma,
            pltpu.SemaphoreType.REGULAR,
        ],
        compiler_params=pltpu.CompilerParams(
            collective_id=0, has_side_effects=True, vmem_limit_bytes=60 * 1024 * 1024
        ),
        name="register_merge",
    )(*small, moving, fixed, table)
    return pl.pallas_call(
        finish_kernel,
        out_shape=(
            jax.ShapeDtypeStruct((2, STRIPS), F32),
            jax.ShapeDtypeStruct((OWNED, BAND, W), F32),
        ),
        in_specs=[vmem, vmem],
        out_specs=(vmem, vmem),
        name="finish_blocks",
    )(found, owned)


def solution(mesh):
    both = ("slab", "tile")
    placed = (
        P(both, None, None),
        P(None, both, None, None),
        P(None, both),
        P(None, both),
        P(None, None, both),
        P(both),
        P(both),
    )
    return jax.shard_map(
        functools.partial(local, mesh.shape["slab"], mesh.shape["tile"]),
        mesh=mesh,
        in_specs=placed,
        out_specs=(P(None, both), P(both, None, None)),
        check_vma=False,
    )
```

```python
import functools
import math

import jax
import jax.numpy as jnp
import ml_dtypes
import numpy as np
from jax import lax
from jax.experimental import pallas as pl
from jax.experimental.pallas import tpu as pltpu
from jax.sharding import PartitionSpec as P

MESH = pl.DeviceIdType.MESH
F32 = jnp.float32
BF16 = jnp.bfloat16
H = 512
W = 128
STRIPS = 4
PIECES = 16
BAND = H // PIECES
OWNED = 16
HALF = H // 2
QUARTER = HALF // 2
SPEC = HALF + 8
PAD = BAND + 8
RING = 4
GROUP = 2 * BAND
HALF_LANES = W // 2
SHARE = PIECES // 2
PARTS = 1
FIRST = HALF + 16


def tables():
    n = np.arange(HALF)
    even = np.arange(0, HALF, 2)
    odd = np.arange(1, HALF, 2)
    row_scale = 1.0 / math.sqrt(H)

    def cos_rows(k):
        return np.cos(2 * np.pi * ((k[:, None] * n[None, :]) % H) / H) * row_scale

    def sin_rows(k):
        return np.sin(2 * np.pi * ((k[:, None] * n[None, :]) % H) / H) * row_scale

    last = np.zeros((16, HALF))
    last[0] = np.where(n % 2 == 0, 1.0, -1.0) * row_scale
    forward_even = np.concatenate([cos_rows(even), last, -sin_rows(even)], 0)
    forward_odd = np.concatenate([cos_rows(odd), -sin_rows(odd)], 0)
    re_part = 2 * cos_rows(even)
    re_part[0] *= 0.5
    im_part = -2 * sin_rows(even)
    im_part[0] = last[0]
    back_even = np.concatenate([re_part, im_part], 0).T
    back_odd = np.concatenate([2 * cos_rows(odd), -2 * sin_rows(odd)], 0).T
    m = np.arange(W)
    angle = 2 * np.pi * ((m[:, None] * m[None, :]) % W) / W
    c, s = np.cos(angle) / math.sqrt(W), np.sin(angle) / math.sqrt(W)
    column_forward = np.block([[c, -s], [s, c]])
    column_back = np.block([[c, s], [-s, c]])
    table = np.concatenate(
        [forward_even, forward_odd, column_forward, column_back, back_even, back_odd], 0
    )
    high = table.astype(ml_dtypes.bfloat16)
    low = (table - high.astype(np.float64)).astype(ml_dtypes.bfloat16)
    return jnp.asarray(np.stack([high, low]))


TABLE_ROWS = FIRST + 5 * HALF


def dot(a, b):
    return jnp.dot(a, b, preferred_element_type=F32)


def split(x):
    high = x.astype(BF16)
    return high, (x - high.astype(F32)).astype(BF16)


def part(table, index):
    start, rows = (0, FIRST) if index == 0 else (FIRST + HALF * (index - 1), HALF)
    return table[0, start : start + rows, :], table[1, start : start + rows, :]


def left(table, index, x):
    high, low = part(table, index)
    xh, xl = split(x)
    return dot(high, xh) + (dot(low, xh) + dot(high, xl))


def right(x, table, index):
    high, low = part(table, index)
    xh, xl = split(x)
    return dot(xh, high) + (dot(xl, high) + dot(xh, low))


def forward_pair(table, a, b):
    x = jnp.concatenate([a, b], 1)
    u = left(table, 0, x[:HALF] + x[HALF:])
    v = left(table, 1, x[:HALF] - x[HALF:])
    joined = []
    for i in range(2):
        lanes = slice(W * i, W * (i + 1))
        re_part = jnp.concatenate(
            [u[:QUARTER, lanes], v[:QUARTER, lanes], u[QUARTER : QUARTER + 8, lanes]], 0)
        im_part = jnp.concatenate(
            [u[QUARTER + 16 :, lanes], v[QUARTER:, lanes], jnp.zeros((8, W), F32)], 0)
        joined.append(jnp.concatenate([re_part, im_part], 1))
    return right(jnp.concatenate(joined, 0), table, 2)


def surfaces(table, fixed_spectrum, spectra):
    fr, fi = fixed_spectrum[:, :W], fixed_spectrum[:, W:]
    crossed = []
    for i in range(2):
        gr, gi = spectra[SPEC * i : SPEC * (i + 1), :W], spectra[SPEC * i : SPEC * (i + 1), W:]
        cr = fr * gr + fi * gi
        ci = fi * gr - fr * gi
        scale = lax.rsqrt(cr * cr + ci * ci + 0.0625)
        crossed.append(jnp.concatenate([cr * scale, ci * scale], 1))
    back = right(jnp.concatenate(crossed, 0), table, 3)
    evens, odds = [], []
    first = lax.broadcasted_iota(jnp.int32, (8, W), 0) == 0
    for i in range(2):
        pr, pi = back[SPEC * i : SPEC * (i + 1), :W], back[SPEC * i : SPEC * (i + 1), W:]
        evens.append(jnp.concatenate(
            [pr[:QUARTER], jnp.where(first, pr[HALF:], pi[:8]), pi[8:QUARTER]], 0))
        odds.append(jnp.concatenate([pr[QUARTER:HALF], pi[QUARTER:HALF]], 0))
    even = left(table, 4, jnp.concatenate(evens, 1))
    odd = left(table, 5, jnp.concatenate(odds, 1))
    return even + jnp.abs(odd)


def shuffled(outer, inner, whole=False):
    pairs = [(j, i) for j in range(outer) for i in range(inner) if whole or j or i]
    order = np.random.default_rng(7).permutation(len(pairs))
    return [pairs[k] for k in order]


def far_first(*sizes):
    grid = [[]]
    for size in sizes:
        grid = [g + [v] for g in grid for v in range(size)]
    grid = [tuple(g) for g in grid if any(g)]

    def hops(g):
        return sum(min(v, RING - v) for v in g[:-1]) + (
            min(g[-1], RING - g[-1]) if sizes[-1] == RING else 0.25 * g[-1])

    return sorted(grid, key=lambda g: (-hops(g), g))


def whole_kernel(
    slabs, tiles, dest_in, slot_in, shifts_in, live, block_in, moving, fixed_in, table_in,
    peaks, owned, dest, slot, shifts, block, fixed, table, gots, pick0, pick1, partner, code0, code1, inv_v, inv_s, fixed_spec,
    merged, spread, rows_got, label_got, onehot, sums, packed,
    send_sem, spread_sem, code_sem, label_sem, slot_sem, rows_sem, own_sem, owner_sem, ready,
):
    p = lax.axis_index("slab")
    q = lax.axis_index("tile")
    z, x = p // RING, lax.rem(p, RING)
    y, c = q // 2, lax.rem(q, 2)
    me = p * tiles + q
    member = lax.rem(me, GROUP)
    devices = slabs * tiles
    axes = ("slab", "tile")
    sizes = (slabs, tiles)
    mine = (p, q)
    got = (gots[:PARTS], gots[PARTS:])
    pick = (pick0, pick1)
    code = (code0, code1)
    rows = (H // slabs, H // tiles)

    def slab_peer(g):
        return lax.rem(z + g[0], RING) * RING + lax.rem(x + g[1], RING)

    def tile_peer(g):
        return lax.rem(y + g[0], RING) * 2 + lax.rem(c + g[1], 2)

    peers = (
        [slab_peer(g) for g in far_first(RING, RING)],
        [tile_peer(g) for g in far_first(RING, 2)],
    )

    def local_wait(ref, sem):
        pltpu.make_async_copy(ref, ref, sem).wait()

    row8 = lax.broadcasted_iota(jnp.int32, (8, W), 0)
    lane8 = lax.broadcasted_iota(jnp.int32, (8, W), 1)

    barrier = pltpu.get_barrier_semaphore()
    for r in range(2):
        for peer in peers[r]:
            pl.semaphore_signal(barrier, inc=1, device_id={axes[r]: peer}, device_id_type=MESH)
    small = [
        pltpu.make_async_copy(a, b, own_sem.at[5 + i])
        for i, (a, b) in enumerate((
            (dest_in, dest), (slot_in, slot), (shifts_in, shifts), (block_in, block)))
    ]
    for copy in small:
        copy.start()
    for copy in small:
        copy.wait()
    for r in range(2):
        tile = jnp.full((8, W), -1, jnp.int32)
        for s in range(STRIPS):
            tile = jnp.where(row8 == s, dest[r, s] * STRIPS + slot[r, s], tile)
        code[r][mine[r]] = tile
    tile = jnp.zeros((8, W), jnp.int32)
    for s in range(STRIPS):
        for k in range(PIECES):
            at = (row8 == (k // SHARE) * STRIPS + s) & (lane8 == k % SHARE)
            tile = jnp.where(at, block[s * PIECES + k], tile)
    label_got[member] = pltpu.roll(tile, lax.rem(member, W // SHARE) * SHARE, 1)
    pl.semaphore_wait(barrier, slabs + tiles - 2)

    for r in range(2):
        for peer in peers[r]:
            pltpu.make_async_remote_copy(
                src_ref=code[r].at[mine[r]], dst_ref=code[r].at[mine[r]],
                send_sem=send_sem.at[r], recv_sem=code_sem.at[r],
                device_id={axes[r]: peer}, device_id_type=MESH,
            ).start()

    def chunk_rows(r, at, half):
        part_rows = rows[r] // PARTS
        return pl.ds(pl.multiple_of(at * rows[r] + half * part_rows, part_rows), part_rows)

    def spread_start(r, i, half):
        peer = peers[r][i]
        pltpu.make_async_remote_copy(
            src_ref=moving.at[r, :, chunk_rows(r, peer, half), :],
            dst_ref=got[r][half].at[pl.ds(mine[r] * STRIPS, STRIPS)],
            send_sem=send_sem.at[2 + r], recv_sem=spread_sem.at[r, half],
            device_id={axes[r]: peer}, device_id_type=MESH,
        ).start()

    own = []
    for half in range(PARTS):
        for i in range(slabs - 1):
            spread_start(0, i, half)
            if i % 2 == 0 and i // 2 < tiles - 1:
                spread_start(1, i // 2, half)
        own.append([
            pltpu.make_async_copy(
                moving.at[r, :, chunk_rows(r, mine[r], half), :],
                got[r][half].at[pl.ds(mine[r] * STRIPS, STRIPS)], own_sem.at[PARTS * r + half])
            for r in range(2)
        ])
    load_fixed = pltpu.make_async_copy(fixed_in, fixed, own_sem.at[10])
    load_table = pltpu.make_async_copy(table_in, table, own_sem.at[11])
    load_fixed.start()
    load_table.start()
    for copies in own:
        for copy in copies:
            copy.start()
    for peer in peers[0]:
        pl.semaphore_signal(ready, inc=1, device_id={"slab": peer}, device_id_type=MESH)

    for r in range(2):
        local_wait(code[r].at[pl.ds(0, sizes[r] - 1)], code_sem.at[r])
        total = jnp.zeros((8, W), jnp.int32)
        for i in range(sizes[r]):
            total += jnp.where(code[r][i] == lane8, i * STRIPS + row8, 0)
        source = jnp.minimum(jnp.sum(total, 0, keepdims=True), sizes[r] * STRIPS - 1)
        inv_v[r] = jnp.broadcast_to(source, (8, W))
    to_scalars = pltpu.make_async_copy(inv_v, inv_s, own_sem.at[4])
    to_scalars.start()

    pl.semaphore_wait(ready, slabs - 1)
    group_rows = GROUP // tiles
    group_base = (p // group_rows) * group_rows
    tile_ring = [lax.rem(q + i, tiles) for i in range(tiles)]

    row_ring = [lax.rem(p + j, group_rows) for j in range(group_rows)]

    def to_group(send):
        for j, i in shuffled(group_rows, tiles):
            send(row_ring[j] * tiles + tile_ring[i], (group_base + row_ring[j], tile_ring[i]))

    def send_label(peer, device):
        pltpu.make_async_remote_copy(
            src_ref=label_got.at[member], dst_ref=label_got.at[member],
            send_sem=send_sem.at[4], recv_sem=label_sem,
            device_id=device, device_id_type=MESH,
        ).start()

    to_group(send_label)

    load_fixed.wait()
    load_table.wait()

    def fixed_pair(i, carry):
        spectra = forward_pair(table, fixed[2 * i], fixed[2 * i + 1])
        fixed_spec[2 * i] = spectra[:SPEC]
        fixed_spec[2 * i + 1] = spectra[SPEC:]
        return carry

    lax.fori_loop(0, STRIPS // 2, fixed_pair, 0)

    local_wait(label_got.at[pl.ds(0, GROUP - 1)], label_sem)
    columns = []
    for g in range(GROUP * SHARE // W):
        total = label_got[W // SHARE * g]
        for d in range(1, W // SHARE):
            total = total + label_got[W // SHARE * g + d]
        columns.append(total)
    chunk = 256

    def build_slot(s):
        def build(i, carry):
            want = lax.broadcasted_iota(jnp.int32, (chunk, W), 0) + i * chunk
            for half in range(2):
                for g, column in enumerate(columns):
                    at = half * STRIPS + s
                    hit = jnp.broadcast_to(column[at : at + 1], (chunk, W)) == want
                    lanes = W * (len(columns) * half + g)
                    onehot[s, pl.ds(pl.multiple_of(i * chunk, chunk), chunk), lanes : lanes + W] = (
                        jnp.where(hit, 1.0, 0.0).astype(BF16))
            return carry

        lax.fori_loop(0, devices * OWNED // chunk, build, 0)

    build_slot(0)
    build_slot(1)

    to_scalars.wait()

    turns = sorted(
        ((r, i) for r in range(2) for i in range(len(peers[r]))),
        key=lambda turn: (turn[1] / len(peers[turn[0]]), turn[0]))

    def second(half):
        for r in (1, 0):
            own[half][r].wait()
            local_wait(got[r][half].at[pl.ds(0, (sizes[r] - 1) * STRIPS)], spread_sem.at[r, half])

        def choose(s, carry):
            for r in (0, 1):
                place = chunk_rows(r, mine[r], half)
                partner[r, s, place, :] = got[r][half][inv_s[r, 0, mine[r] * STRIPS + s]]
                for peer in peers[r]:
                    pick[r][half, s, peer] = got[r][half][inv_s[r, 0, peer * STRIPS + s]]
            for r, i in turns:
                place = chunk_rows(r, mine[r], half)
                peer = peers[r][i]
                pltpu.make_async_remote_copy(
                    src_ref=pick[r].at[half, s, peer], dst_ref=partner.at[r, s, place, :],
                    send_sem=send_sem.at[5 + r], recv_sem=slot_sem.at[r, s],
                    device_id={axes[r]: peer}, device_id_type=MESH,
                ).start()
            return carry

        lax.fori_loop(0, STRIPS, choose, 0)

    second(0)
    build_slot(2)
    build_slot(3)
    for half in range(1, PARTS):
        second(half)

    low_half = lane8 < HALF_LANES

    def correlate(s, found):
        for r in range(2):
            local_wait(partner.at[r, s, pl.ds(0, H - rows[r])], slot_sem.at[r, s])
        spectra = forward_pair(table, partner[0, s], partner[1, s])
        surface = surfaces(table, fixed_spec[s], spectra)
        is_live = s < live[0]
        total = jnp.ones((1, 1), F32)
        acc = fixed[s]
        for r in range(2):
            peak = jnp.max(surface[:, W * r : W * (r + 1)], axis=(0, 1), keepdims=True)
            weight = 1.0 / (1.0 + jnp.exp(4.0 - peak))
            down = lax.rem(shifts[r, 0, s] + H, H)
            side = lax.rem(shifts[r, 1, s] + W, W)
            moved = pltpu.roll(pltpu.roll(partner[r, s], side, 1), down, 0)
            acc = acc + weight * moved
            total = total + weight
            shown = jnp.where(is_live, peak, 0.0)
            found = jnp.where((row8 == r) & (lane8 == s), shown, found)
        acc = jnp.where(is_live, acc * (1.0 / total), 0.0)
        for k in range(PIECES):
            merged[pl.ds(k * PAD, BAND), :] = acc[k * BAND : (k + 1) * BAND]
        for r in range(BAND):
            top = merged[pl.ds(r, SHARE, stride=PAD), :]
            bottom = merged[pl.ds(r + SHARE * PAD, SHARE, stride=PAD), :]
            spread[s, 2 * r] = jnp.where(low_half, top, pltpu.roll(bottom, HALF_LANES, 1))
            spread[s, 2 * r + 1] = jnp.where(low_half, pltpu.roll(top, HALF_LANES, 1), bottom)
        rows_got[s, member] = spread[s, member]

        def send_rows(peer, device):
            pltpu.make_async_remote_copy(
                src_ref=spread.at[s, peer], dst_ref=rows_got.at[s, member],
                send_sem=send_sem.at[7], recv_sem=rows_sem.at[s],
                device_id=device, device_id_type=MESH,
            ).start()

        to_group(send_rows)
        return found

    found = lax.fori_loop(0, STRIPS, correlate, jnp.zeros((8, W), F32))
    peaks[...] = found

    big = 1024
    plane_rows = RING * tiles * OWNED
    low_rows = lax.broadcasted_iota(jnp.int32, (GROUP * SHARE, W), 1) < HALF_LANES

    def send_owner(op, oq):
        pltpu.make_async_remote_copy(
            src_ref=packed.at[op * tiles + oq], dst_ref=owned.at[me],
            send_sem=send_sem.at[8], recv_sem=owner_sem,
            device_id=(op, oq), device_id_type=MESH,
        ).start()

    for s in range(STRIPS):
        local_wait(rows_got.at[s, pl.ds(0, GROUP - 1)], rows_sem.at[s])
        rows_here = rows_got[s].reshape(GROUP * SHARE, W)
        high = rows_here.astype(BF16).astype(F32)
        low = rows_here - high
        both = jnp.concatenate([
            jnp.where(low_rows, high, pltpu.roll(low, HALF_LANES, 1)),
            jnp.where(low_rows, pltpu.roll(high, HALF_LANES, 1), low),
        ], 0).astype(BF16)
        if s < STRIPS - 1:
            def add(i, carry):
                at = pl.ds(pl.multiple_of(i * big, big), big)
                total = dot(onehot[s, at, :], both)
                sums[at, :] = total if s == 0 else total + sums[at, :]
                return carry

            lax.fori_loop(0, devices * OWNED // big, add, 0)
        else:
            for i in range(RING):
                oz = lax.rem(z + 2 + i, RING)
                at = pl.ds(pl.multiple_of(oz * plane_rows, plane_rows), plane_rows)
                total = dot(onehot[s, at, :], both) + sums[at, :]
                total = (total + pltpu.roll(total, HALF_LANES, 1)).reshape(RING * tiles, 2, 8, W)
                packed[pl.ds(oz * RING * tiles, RING * tiles)] = jnp.where(
                    low_half[None], total[:, 0], total[:, 1])
                for dx, dq in shuffled(RING, tiles, i != 2):
                    send_owner(oz * RING + lax.rem(x + dx, RING), tile_ring[dq])

    last = pltpu.make_async_copy(packed.at[me], owned.at[me], own_sem.at[4])
    last.start()

    for r in range(2):
        local_wait(code[r].at[pl.ds(0, sizes[r] - 1)], send_sem.at[r])
        local_wait(pick[r].at[:, :, pl.ds(0, sizes[r] - 1)], send_sem.at[2 + r])
        local_wait(pick[r].at[:, :, pl.ds(0, sizes[r] - 1)], send_sem.at[5 + r])
    local_wait(label_got.at[pl.ds(0, GROUP - 1)], send_sem.at[4])
    local_wait(spread.at[:, pl.ds(0, GROUP - 1)], send_sem.at[7])

    last.wait()
    local_wait(packed.at[pl.ds(0, devices - 1)], owner_sem)
    local_wait(packed.at[pl.ds(0, devices - 1)], send_sem.at[8])


def finish_kernel(found, owned, peaks, out):
    peaks[...] = found[:2, :STRIPS]
    low_half = lax.broadcasted_iota(jnp.int32, (8, W), 1) < HALF_LANES
    for r in range(BAND):
        a, b = owned[2 * r], owned[2 * r + 1]
        for k in range(1, owned.shape[0] // GROUP):
            a = a + owned[k * GROUP + 2 * r]
            b = b + owned[k * GROUP + 2 * r + 1]
        out[:8, r, :] = jnp.where(low_half, a, pltpu.roll(b, HALF_LANES, 1))
        out[8:, r, :] = jnp.where(low_half, pltpu.roll(a, HALF_LANES, 1), b)


def local(slabs, tiles, fixed, moving, pair_dest, pair_slot, plane_shift, live_count, piece_block):
    table = tables()
    devices = slabs * tiles
    vmem = pl.BlockSpec(memory_space=pltpu.VMEM)
    anywhere = pl.BlockSpec(memory_space=pl.ANY)
    dma = pltpu.SemaphoreType.DMA
    small = (pair_dest, pair_slot, plane_shift, live_count, piece_block)
    found, owned = pl.pallas_call(
        functools.partial(whole_kernel, slabs, tiles),
        out_shape=(
            jax.ShapeDtypeStruct((8, W), F32),
            jax.ShapeDtypeStruct((devices, 8, W), F32),
        ),
        in_specs=[anywhere] * 3 + [pl.BlockSpec(memory_space=pltpu.SMEM)] + [anywhere] * 4,
        out_specs=(vmem, anywhere),
        scratch_shapes=[pltpu.SMEM(a.shape, jnp.int32) for a in small if a.shape != (1,)]
        + [
            pltpu.VMEM((STRIPS, H, W), F32),
            pltpu.VMEM((2, TABLE_ROWS, HALF), BF16),
            [pltpu.VMEM((slabs * STRIPS, H // slabs // PARTS, W), F32)] * PARTS
            + [pltpu.VMEM((tiles * STRIPS, H // tiles // PARTS, W), F32)] * PARTS,
            pltpu.VMEM((PARTS, STRIPS, slabs, H // slabs // PARTS, W), F32),
            pltpu.VMEM((PARTS, STRIPS, tiles, H // tiles // PARTS, W), F32),
            pltpu.VMEM((2, STRIPS, H, W), F32),
            pltpu.VMEM((slabs, 8, W), jnp.int32),
            pltpu.VMEM((tiles, 8, W), jnp.int32),
            pltpu.VMEM((2, 8, W), jnp.int32),
            pltpu.SMEM((2, 8, W), jnp.int32),
            pltpu.VMEM((STRIPS, SPEC, 2 * W), F32),
            pltpu.VMEM((PIECES * PAD, W), F32),
            pltpu.VMEM((STRIPS, GROUP, SHARE, W), F32),
            pltpu.VMEM((STRIPS, GROUP, SHARE, W), F32),
            pltpu.VMEM((GROUP, 8, W), jnp.int32),
            pltpu.VMEM((STRIPS, devices * OWNED, GROUP * PIECES), BF16),
            pltpu.VMEM((devices * OWNED, W), F32),
            pltpu.VMEM((devices, 8, W), F32),
            dma((9,)), dma((2, PARTS)), dma((2,)), dma, dma((2, STRIPS)), dma((STRIPS,)), dma((12,)), dma,
            pltpu.SemaphoreType.REGULAR,
        ],
        compiler_params=pltpu.CompilerParams(
            collective_id=0, has_side_effects=True, vmem_limit_bytes=60 * 1024 * 1024
        ),
        name="register_merge",
    )(*small, moving, fixed, table)
    return pl.pallas_call(
        finish_kernel,
        out_shape=(
            jax.ShapeDtypeStruct((2, STRIPS), F32),
            jax.ShapeDtypeStruct((OWNED, BAND, W), F32),
        ),
        in_specs=[vmem, vmem],
        out_specs=(vmem, vmem),
        name="finish_blocks",
    )(found, owned)


def solution(mesh):
    both = ("slab", "tile")
    placed = (
        P(both, None, None),
        P(None, both, None, None),
        P(None, both),
        P(None, both),
        P(None, None, both),
        P(both),
        P(both),
    )
    return jax.shard_map(
        functools.partial(local, mesh.shape["slab"], mesh.shape["tile"]),
        mesh=mesh,
        in_specs=placed,
        out_specs=(P(None, both), P(both, None, None)),
        check_vma=False,
    )
```

```python
import functools
import math

import jax
import jax.numpy as jnp
import ml_dtypes
import numpy as np
from jax import lax
from jax.experimental import pallas as pl
from jax.experimental.pallas import tpu as pltpu
from jax.sharding import PartitionSpec as P

MESH = pl.DeviceIdType.MESH
F32 = jnp.float32
BF16 = jnp.bfloat16
H = 512
W = 128
STRIPS = 4
PIECES = 16
BAND = H // PIECES
OWNED = 16
HALF = H // 2
QUARTER = HALF // 2
SPEC = HALF + 8
PAD = BAND + 8
RING = 4
GROUP = 2 * BAND
HALF_LANES = W // 2
SHARE = PIECES // 2
PARTS = 1
FIRST = HALF + 16


def tables():
    n = np.arange(HALF)
    even = np.arange(0, HALF, 2)
    odd = np.arange(1, HALF, 2)
    row_scale = 1.0 / math.sqrt(H)

    def cos_rows(k):
        return np.cos(2 * np.pi * ((k[:, None] * n[None, :]) % H) / H) * row_scale

    def sin_rows(k):
        return np.sin(2 * np.pi * ((k[:, None] * n[None, :]) % H) / H) * row_scale

    last = np.zeros((16, HALF))
    last[0] = np.where(n % 2 == 0, 1.0, -1.0) * row_scale
    forward_even = np.concatenate([cos_rows(even), last, -sin_rows(even)], 0)
    forward_odd = np.concatenate([cos_rows(odd), -sin_rows(odd)], 0)
    re_part = 2 * cos_rows(even)
    re_part[0] *= 0.5
    im_part = -2 * sin_rows(even)
    im_part[0] = last[0]
    back_even = np.concatenate([re_part, im_part], 0).T
    back_odd = np.concatenate([2 * cos_rows(odd), -2 * sin_rows(odd)], 0).T
    m = np.arange(W)
    angle = 2 * np.pi * ((m[:, None] * m[None, :]) % W) / W
    c, s = np.cos(angle) / math.sqrt(W), np.sin(angle) / math.sqrt(W)
    column_forward = np.block([[c, -s], [s, c]])
    column_back = np.block([[c, s], [-s, c]])
    table = np.concatenate(
        [forward_even, forward_odd, column_forward, column_back, back_even, back_odd], 0
    )
    high = table.astype(ml_dtypes.bfloat16)
    low = (table - high.astype(np.float64)).astype(ml_dtypes.bfloat16)
    return jnp.asarray(np.stack([high, low]))


TABLE_ROWS = FIRST + 5 * HALF


def dot(a, b):
    return jnp.dot(a, b, preferred_element_type=F32)


def split(x):
    high = x.astype(BF16)
    return high, (x - high.astype(F32)).astype(BF16)


def part(table, index):
    start, rows = (0, FIRST) if index == 0 else (FIRST + HALF * (index - 1), HALF)
    return table[0, start : start + rows, :], table[1, start : start + rows, :]


def left(table, index, x):
    high, low = part(table, index)
    xh, xl = split(x)
    return dot(high, xh) + (dot(low, xh) + dot(high, xl))


def right(x, table, index):
    high, low = part(table, index)
    xh, xl = split(x)
    return dot(xh, high) + (dot(xl, high) + dot(xh, low))


def forward_pair(table, a, b):
    x = jnp.concatenate([a, b], 1)
    u = left(table, 0, x[:HALF] + x[HALF:])
    v = left(table, 1, x[:HALF] - x[HALF:])
    joined = []
    for i in range(2):
        lanes = slice(W * i, W * (i + 1))
        re_part = jnp.concatenate(
            [u[:QUARTER, lanes], v[:QUARTER, lanes], u[QUARTER : QUARTER + 8, lanes]], 0)
        im_part = jnp.concatenate(
            [u[QUARTER + 16 :, lanes], v[QUARTER:, lanes], jnp.zeros((8, W), F32)], 0)
        joined.append(jnp.concatenate([re_part, im_part], 1))
    return right(jnp.concatenate(joined, 0), table, 2)


def surfaces(table, fixed_spectrum, spectra):
    fr, fi = fixed_spectrum[:, :W], fixed_spectrum[:, W:]
    crossed = []
    for i in range(2):
        gr, gi = spectra[SPEC * i : SPEC * (i + 1), :W], spectra[SPEC * i : SPEC * (i + 1), W:]
        cr = fr * gr + fi * gi
        ci = fi * gr - fr * gi
        scale = lax.rsqrt(cr * cr + ci * ci + 0.0625)
        crossed.append(jnp.concatenate([cr * scale, ci * scale], 1))
    back = right(jnp.concatenate(crossed, 0), table, 3)
    evens, odds = [], []
    first = lax.broadcasted_iota(jnp.int32, (8, W), 0) == 0
    for i in range(2):
        pr, pi = back[SPEC * i : SPEC * (i + 1), :W], back[SPEC * i : SPEC * (i + 1), W:]
        evens.append(jnp.concatenate(
            [pr[:QUARTER], jnp.where(first, pr[HALF:], pi[:8]), pi[8:QUARTER]], 0))
        odds.append(jnp.concatenate([pr[QUARTER:HALF], pi[QUARTER:HALF]], 0))
    even = left(table, 4, jnp.concatenate(evens, 1))
    odd = left(table, 5, jnp.concatenate(odds, 1))
    return even + jnp.abs(odd)


def shuffled(outer, inner, whole=False):
    pairs = [(j, i) for j in range(outer) for i in range(inner) if whole or j or i]
    order = np.random.default_rng(7).permutation(len(pairs))
    return [pairs[k] for k in order]


def far_first(*sizes):
    grid = [[]]
    for size in sizes:
        grid = [g + [v] for g in grid for v in range(size)]
    grid = [tuple(g) for g in grid if any(g)]

    def hops(g):
        return sum(min(v, RING - v) for v in g[:-1]) + (
            min(g[-1], RING - g[-1]) if sizes[-1] == RING else 0.25 * g[-1])

    return sorted(grid, key=lambda g: (-hops(g), g))


def whole_kernel(
    slabs, tiles, dest_in, slot_in, shifts_in, live, block_in, moving, fixed_in, table_in,
    peaks, owned, dest, slot, shifts, block, fixed, table, gots, pick0, pick1, partner, code0, code1, inv_v, inv_s, fixed_spec,
    merged, spread, rows_got, label_got, onehot, sums, packed,
    send_sem, spread_sem, code_sem, label_sem, slot_sem, rows_sem, own_sem, owner_sem, ready,
):
    p = lax.axis_index("slab")
    q = lax.axis_index("tile")
    z, x = p // RING, lax.rem(p, RING)
    y, c = q // 2, lax.rem(q, 2)
    me = p * tiles + q
    member = lax.rem(me, GROUP)
    devices = slabs * tiles
    axes = ("slab", "tile")
    sizes = (slabs, tiles)
    mine = (p, q)
    got = (gots[:PARTS], gots[PARTS:])
    pick = (pick0, pick1)
    code = (code0, code1)
    rows = (H // slabs, H // tiles)

    def slab_peer(g):
        return lax.rem(z + g[0], RING) * RING + lax.rem(x + g[1], RING)

    def tile_peer(g):
        return lax.rem(y + g[0], RING) * 2 + lax.rem(c + g[1], 2)

    peers = (
        [slab_peer(g) for g in far_first(RING, RING)],
        [tile_peer(g) for g in far_first(RING, 2)],
    )

    def local_wait(ref, sem):
        pltpu.make_async_copy(ref, ref, sem).wait()

    row8 = lax.broadcasted_iota(jnp.int32, (8, W), 0)
    lane8 = lax.broadcasted_iota(jnp.int32, (8, W), 1)

    barrier = pltpu.get_barrier_semaphore()
    for r in range(2):
        for peer in peers[r]:
            pl.semaphore_signal(barrier, inc=1, device_id={axes[r]: peer}, device_id_type=MESH)
    small = [
        pltpu.make_async_copy(a, b, own_sem.at[5 + i])
        for i, (a, b) in enumerate((
            (dest_in, dest), (slot_in, slot), (shifts_in, shifts), (block_in, block)))
    ]
    for copy in small:
        copy.start()
    for copy in small:
        copy.wait()
    for r in range(2):
        tile = jnp.full((8, W), -1, jnp.int32)
        for s in range(STRIPS):
            tile = jnp.where(row8 == s, dest[r, s] * STRIPS + slot[r, s], tile)
        code[r][mine[r]] = tile
    tile = jnp.zeros((8, W), jnp.int32)
    for s in range(STRIPS):
        for k in range(PIECES):
            at = (row8 == (k // SHARE) * STRIPS + s) & (lane8 == k % SHARE)
            tile = jnp.where(at, block[s * PIECES + k], tile)
    label_got[member] = pltpu.roll(tile, lax.rem(member, W // SHARE) * SHARE, 1)
    pl.semaphore_wait(barrier, slabs + tiles - 2)

    for r in range(2):
        for peer in peers[r]:
            pltpu.make_async_remote_copy(
                src_ref=code[r].at[mine[r]], dst_ref=code[r].at[mine[r]],
                send_sem=send_sem.at[r], recv_sem=code_sem.at[r],
                device_id={axes[r]: peer}, device_id_type=MESH,
            ).start()

    def chunk_rows(r, at, half):
        part_rows = rows[r] // PARTS
        return pl.ds(pl.multiple_of(at * rows[r] + half * part_rows, part_rows), part_rows)

    def spread_start(r, i, half):
        peer = peers[r][i]
        pltpu.make_async_remote_copy(
            src_ref=moving.at[r, :, chunk_rows(r, peer, half), :],
            dst_ref=got[r][half].at[pl.ds(mine[r] * STRIPS, STRIPS)],
            send_sem=send_sem.at[2 + r], recv_sem=spread_sem.at[r, half],
            device_id={axes[r]: peer}, device_id_type=MESH,
        ).start()

    own = []
    for half in range(PARTS):
        for i in range(slabs - 1):
            spread_start(0, i, half)
            if i % 2 == 0 and i // 2 < tiles - 1:
                spread_start(1, i // 2, half)
        own.append([
            pltpu.make_async_copy(
                moving.at[r, :, chunk_rows(r, mine[r], half), :],
                got[r][half].at[pl.ds(mine[r] * STRIPS, STRIPS)], own_sem.at[PARTS * r + half])
            for r in range(2)
        ])
    load_fixed = pltpu.make_async_copy(fixed_in, fixed, own_sem.at[10])
    load_table = pltpu.make_async_copy(table_in, table, own_sem.at[11])
    load_fixed.start()
    load_table.start()
    for copies in own:
        for copy in copies:
            copy.start()
    for peer in peers[0]:
        pl.semaphore_signal(ready, inc=1, device_id={"slab": peer}, device_id_type=MESH)

    for r in range(2):
        local_wait(code[r].at[pl.ds(0, sizes[r] - 1)], code_sem.at[r])
        total = jnp.zeros((8, W), jnp.int32)
        for i in range(sizes[r]):
            total += jnp.where(code[r][i] == lane8, i * STRIPS + row8, 0)
        source = jnp.minimum(jnp.sum(total, 0, keepdims=True), sizes[r] * STRIPS - 1)
        inv_v[r] = jnp.broadcast_to(source, (8, W))
    to_scalars = pltpu.make_async_copy(inv_v, inv_s, own_sem.at[4])
    to_scalars.start()

    pl.semaphore_wait(ready, slabs - 1)
    group_rows = GROUP // tiles
    group_base = (p // group_rows) * group_rows
    tile_ring = [lax.rem(q + i, tiles) for i in range(tiles)]

    row_ring = [lax.rem(p + j, group_rows) for j in range(group_rows)]

    def to_group(send):
        for j, i in shuffled(group_rows, tiles):
            send(row_ring[j] * tiles + tile_ring[i], (group_base + row_ring[j], tile_ring[i]))

    def send_label(peer, device):
        pltpu.make_async_remote_copy(
            src_ref=label_got.at[member], dst_ref=label_got.at[member],
            send_sem=send_sem.at[4], recv_sem=label_sem,
            device_id=device, device_id_type=MESH,
        ).start()

    to_group(send_label)

    load_fixed.wait()
    load_table.wait()

    def fixed_pair(i, carry):
        spectra = forward_pair(table, fixed[2 * i], fixed[2 * i + 1])
        fixed_spec[2 * i] = spectra[:SPEC]
        fixed_spec[2 * i + 1] = spectra[SPEC:]
        return carry

    lax.fori_loop(0, STRIPS // 2, fixed_pair, 0)

    local_wait(label_got.at[pl.ds(0, GROUP - 1)], label_sem)
    columns = []
    for g in range(GROUP * SHARE // W):
        total = label_got[W // SHARE * g]
        for d in range(1, W // SHARE):
            total = total + label_got[W // SHARE * g + d]
        columns.append(total)
    chunk = 256

    def build_slot(s):
        def build(i, carry):
            want = lax.broadcasted_iota(jnp.int32, (chunk, W), 0) + i * chunk
            for half in range(2):
                for g, column in enumerate(columns):
                    at = half * STRIPS + s
                    hit = jnp.broadcast_to(column[at : at + 1], (chunk, W)) == want
                    lanes = W * (len(columns) * half + g)
                    onehot[s, pl.ds(pl.multiple_of(i * chunk, chunk), chunk), lanes : lanes + W] = (
                        jnp.where(hit, 1.0, 0.0).astype(BF16))
            return carry

        lax.fori_loop(0, devices * OWNED // chunk, build, 0)

    build_slot(0)
    build_slot(1)

    to_scalars.wait()

    turns = sorted(
        ((r, i) for r in range(2) for i in range(len(peers[r]))),
        key=lambda turn: (turn[1] / len(peers[turn[0]]), turn[0]))

    def second(half):
        for r in (1, 0):
            own[half][r].wait()
            local_wait(got[r][half].at[pl.ds(0, (sizes[r] - 1) * STRIPS)], spread_sem.at[r, half])

        def choose(s, carry):
            for r in (0, 1):
                place = chunk_rows(r, mine[r], half)
                partner[r, s, place, :] = got[r][half][inv_s[r, 0, mine[r] * STRIPS + s]]
                for peer in peers[r]:
                    pick[r][half, s, peer] = got[r][half][inv_s[r, 0, peer * STRIPS + s]]
            for r, i in turns:
                place = chunk_rows(r, mine[r], half)
                peer = peers[r][i]
                pltpu.make_async_remote_copy(
                    src_ref=pick[r].at[half, s, peer], dst_ref=partner.at[r, s, place, :],
                    send_sem=send_sem.at[5 + r], recv_sem=slot_sem.at[r, s],
                    device_id={axes[r]: peer}, device_id_type=MESH,
                ).start()
            return carry

        lax.fori_loop(0, STRIPS, choose, 0)

    second(0)
    build_slot(2)
    build_slot(3)
    for half in range(1, PARTS):
        second(half)

    low_half = lane8 < HALF_LANES

    def correlate(s, found):
        for r in range(2):
            local_wait(partner.at[r, s, pl.ds(0, H - rows[r])], slot_sem.at[r, s])
        spectra = forward_pair(table, partner[0, s], partner[1, s])
        surface = surfaces(table, fixed_spec[s], spectra)
        is_live = s < live[0]
        total = jnp.ones((1, 1), F32)
        acc = fixed[s]
        for r in range(2):
            peak = jnp.max(surface[:, W * r : W * (r + 1)], axis=(0, 1), keepdims=True)
            weight = 1.0 / (1.0 + jnp.exp(4.0 - peak))
            down = lax.rem(shifts[r, 0, s] + H, H)
            side = lax.rem(shifts[r, 1, s] + W, W)
            moved = pltpu.roll(pltpu.roll(partner[r, s], side, 1), down, 0)
            acc = acc + weight * moved
            total = total + weight
            shown = jnp.where(is_live, peak, 0.0)
            found = jnp.where((row8 == r) & (lane8 == s), shown, found)
        acc = jnp.where(is_live, acc * (1.0 / total), 0.0)
        for k in range(PIECES):
            merged[pl.ds(k * PAD, BAND), :] = acc[k * BAND : (k + 1) * BAND]
        for r in range(BAND):
            top = merged[pl.ds(r, SHARE, stride=PAD), :]
            bottom = merged[pl.ds(r + SHARE * PAD, SHARE, stride=PAD), :]
            spread[s, 2 * r] = jnp.where(low_half, top, pltpu.roll(bottom, HALF_LANES, 1))
            spread[s, 2 * r + 1] = jnp.where(low_half, pltpu.roll(top, HALF_LANES, 1), bottom)
        rows_got[s, member] = spread[s, member]

        def send_rows(peer, device):
            pltpu.make_async_remote_copy(
                src_ref=spread.at[s, peer], dst_ref=rows_got.at[s, member],
                send_sem=send_sem.at[7], recv_sem=rows_sem.at[s],
                device_id=device, device_id_type=MESH,
            ).start()

        to_group(send_rows)
        return found

    found = lax.fori_loop(0, STRIPS, correlate, jnp.zeros((8, W), F32))
    peaks[...] = found

    big = 1024
    plane_rows = RING * tiles * OWNED
    low_rows = lax.broadcasted_iota(jnp.int32, (GROUP * SHARE, W), 1) < HALF_LANES

    def send_owner(op, oq):
        pltpu.make_async_remote_copy(
            src_ref=packed.at[op * tiles + oq], dst_ref=owned.at[me],
            send_sem=send_sem.at[8], recv_sem=owner_sem,
            device_id=(op, oq), device_id_type=MESH,
        ).start()

    for s in range(STRIPS):
        local_wait(rows_got.at[s, pl.ds(0, GROUP - 1)], rows_sem.at[s])
        rows_here = rows_got[s].reshape(GROUP * SHARE, W)
        high = rows_here.astype(BF16).astype(F32)
        low = rows_here - high
        both = jnp.concatenate([
            jnp.where(low_rows, high, pltpu.roll(low, HALF_LANES, 1)),
            jnp.where(low_rows, pltpu.roll(high, HALF_LANES, 1), low),
        ], 0).astype(BF16)
        if s < STRIPS - 1:
            def add(i, carry):
                at = pl.ds(pl.multiple_of(i * big, big), big)
                total = dot(onehot[s, at, :], both)
                sums[at, :] = total if s == 0 else total + sums[at, :]
                return carry

            lax.fori_loop(0, devices * OWNED // big, add, 0)
        else:
            for i in range(RING):
                oz = lax.rem(z + 2 + i, RING)
                at = pl.ds(pl.multiple_of(oz * plane_rows, plane_rows), plane_rows)
                total = dot(onehot[s, at, :], both) + sums[at, :]
                total = (total + pltpu.roll(total, HALF_LANES, 1)).reshape(RING * tiles, 2, 8, W)
                packed[pl.ds(oz * RING * tiles, RING * tiles)] = jnp.where(
                    low_half[None], total[:, 0], total[:, 1])
                for dx, dq in shuffled(RING, tiles, i != 2):
                    send_owner(oz * RING + lax.rem(x + dx, RING), tile_ring[dq])

    owned[me] = packed[me]

    for r in range(2):
        local_wait(code[r].at[pl.ds(0, sizes[r] - 1)], send_sem.at[r])
        local_wait(pick[r].at[:, :, pl.ds(0, sizes[r] - 1)], send_sem.at[2 + r])
        local_wait(pick[r].at[:, :, pl.ds(0, sizes[r] - 1)], send_sem.at[5 + r])
    local_wait(label_got.at[pl.ds(0, GROUP - 1)], send_sem.at[4])
    local_wait(spread.at[:, pl.ds(0, GROUP - 1)], send_sem.at[7])

    local_wait(packed.at[pl.ds(0, devices - 1)], owner_sem)
    local_wait(packed.at[pl.ds(0, devices - 1)], send_sem.at[8])


def finish_kernel(found, owned, peaks, out):
    peaks[...] = found[:2, :STRIPS]
    low_half = lax.broadcasted_iota(jnp.int32, (8, W), 1) < HALF_LANES
    for r in range(BAND):
        a, b = owned[2 * r], owned[2 * r + 1]
        for k in range(1, owned.shape[0] // GROUP):
            a = a + owned[k * GROUP + 2 * r]
            b = b + owned[k * GROUP + 2 * r + 1]
        out[:8, r, :] = jnp.where(low_half, a, pltpu.roll(b, HALF_LANES, 1))
        out[8:, r, :] = jnp.where(low_half, pltpu.roll(a, HALF_LANES, 1), b)


def local(slabs, tiles, fixed, moving, pair_dest, pair_slot, plane_shift, live_count, piece_block):
    table = tables()
    devices = slabs * tiles
    vmem = pl.BlockSpec(memory_space=pltpu.VMEM)
    anywhere = pl.BlockSpec(memory_space=pl.ANY)
    dma = pltpu.SemaphoreType.DMA
    small = (pair_dest, pair_slot, plane_shift, live_count, piece_block)
    found, owned = pl.pallas_call(
        functools.partial(whole_kernel, slabs, tiles),
        out_shape=(
            jax.ShapeDtypeStruct((8, W), F32),
            jax.ShapeDtypeStruct((devices, 8, W), F32),
        ),
        in_specs=[anywhere] * 3 + [pl.BlockSpec(memory_space=pltpu.SMEM)] + [anywhere] * 4,
        out_specs=(vmem, vmem),
        scratch_shapes=[pltpu.SMEM(a.shape, jnp.int32) for a in small if a.shape != (1,)]
        + [
            pltpu.VMEM((STRIPS, H, W), F32),
            pltpu.VMEM((2, TABLE_ROWS, HALF), BF16),
            [pltpu.VMEM((slabs * STRIPS, H // slabs // PARTS, W), F32)] * PARTS
            + [pltpu.VMEM((tiles * STRIPS, H // tiles // PARTS, W), F32)] * PARTS,
            pltpu.VMEM((PARTS, STRIPS, slabs, H // slabs // PARTS, W), F32),
            pltpu.VMEM((PARTS, STRIPS, tiles, H // tiles // PARTS, W), F32),
            pltpu.VMEM((2, STRIPS, H, W), F32),
            pltpu.VMEM((slabs, 8, W), jnp.int32),
            pltpu.VMEM((tiles, 8, W), jnp.int32),
            pltpu.VMEM((2, 8, W), jnp.int32),
            pltpu.SMEM((2, 8, W), jnp.int32),
            pltpu.VMEM((STRIPS, SPEC, 2 * W), F32),
            pltpu.VMEM((PIECES * PAD, W), F32),
            pltpu.VMEM((STRIPS, GROUP, SHARE, W), F32),
            pltpu.VMEM((STRIPS, GROUP, SHARE, W), F32),
            pltpu.VMEM((GROUP, 8, W), jnp.int32),
            pltpu.VMEM((STRIPS, devices * OWNED, GROUP * PIECES), BF16),
            pltpu.VMEM((devices * OWNED, W), F32),
            pltpu.VMEM((devices, 8, W), F32),
            dma((9,)), dma((2, PARTS)), dma((2,)), dma, dma((2, STRIPS)), dma((STRIPS,)), dma((12,)), dma,
            pltpu.SemaphoreType.REGULAR,
        ],
        compiler_params=pltpu.CompilerParams(
            collective_id=0, has_side_effects=True, vmem_limit_bytes=60 * 1024 * 1024
        ),
        name="register_merge",
    )(*small, moving, fixed, table)
    return pl.pallas_call(
        finish_kernel,
        out_shape=(
            jax.ShapeDtypeStruct((2, STRIPS), F32),
            jax.ShapeDtypeStruct((OWNED, BAND, W), F32),
        ),
        in_specs=[vmem, vmem],
        out_specs=(vmem, vmem),
        name="finish_blocks",
    )(found, owned)


def solution(mesh):
    both = ("slab", "tile")
    placed = (
        P(both, None, None),
        P(None, both, None, None),
        P(None, both),
        P(None, both),
        P(None, None, both),
        P(both),
        P(both),
    )
    return jax.shard_map(
        functools.partial(local, mesh.shape["slab"], mesh.shape["tile"]),
        mesh=mesh,
        in_specs=placed,
        out_specs=(P(None, both), P(both, None, None)),
        check_vma=False,
    )
```
